256 devices in a mesh: gx: 2 (over x_lo), gy: 8 (over x_hi, y), gz: 16 (over z, core).
Axes of the slice: x: 4 (x_hi: 2, x_lo: 2; x = x_hi * 2 + x_lo), y: 4, z: 8, core: 2. Of those that a mesh axis runs over, the one named last changes fastest.
Arguments:
- volume: bfloat16 [32, 64, 64, 256], P(None, 'gx', 'gy', 'gz'), may hold values from -6 to 6
- weight_a: bfloat16 [3, 3, 3, 32, 64], replicated, may hold values from -0.21875 to 0.21875
- bias_a: float32 [64], replicated, may hold values from -3 to 3
- weight_b: bfloat16 [3, 3, 3, 64, 128], replicated, may hold values from -0.15625 to 0.15625
- bias_b: float32 [128], replicated, may hold values from -3 to 3
- cotangent: bfloat16 [128, 32, 32, 128], P(None, ('gx', 'gz'), 'gy'), may hold values from -24 to 24
Outputs:
- features: bfloat16 [128, 32, 32, 128], P(None, ('gx', 'gz'), 'gy')
- grad_input: bfloat16 [32, 64, 64, 256], P(None, 'gx', 'gy', 'gz')
- grad_weight_a: float32 [3, 3, 3, 32, 64], replicated
- grad_bias_a: float32 [64], replicated
- grad_weight_b: float32 [3, 3, 3, 64, 128], replicated
- grad_bias_b: float32 [128], replicated
The draws below stay inside these ranges and needn't reach their ends.
All inputs are finite; a program needn't handle non-finite values.
Results may differ from the reference program's by a relative error of at most 0.012.
Values may be sent and summed in bfloat16 or wider, within the bound.
No kernel may reach another device: no remote copies, remote signals or barrier semaphores. Data moves between devices by JAX's collectives and lax.ppermute only.
A program may use at most 128 MiB of HBM per device.

```python
import math
import jax
import jax.numpy as jnp
from jax import lax

C1 = 32
C2 = 64
C3 = 128
NX = 64
NY = 64
NZ = 256


def level_of(key, dims, shards, least, top_value):
    def one(axis_at, blocks):
        steps = jax.random.uniform(jax.random.fold_in(jax.random.fold_in(key, 6), axis_at), (blocks,), jnp.float32, least / len(shards), top_value / len(shards))
        return jnp.repeat(jnp.exp(steps), dims[axis_at] // blocks).reshape((-1,) + (1,) * (len(dims) - axis_at - 1))

    level = one(*shards[0])
    for cut in shards[1:]:
        level = level * one(*cut)
    return level


def centred(own_key, shape, deviation, limit, cuts=(), dtype=jnp.bfloat16):
    entries = deviation * jax.random.normal(own_key, shape, jnp.float32)
    if cuts:
        entries = entries * level_of(own_key, shape, cuts, -0.22, 0.18)
    return jnp.clip(entries, -limit, limit).astype(dtype)


def setup_inputs(seed: int = 0) -> dict:
    seeds = jax.random.split(jax.random.key(seed), 7)
    return {
        "volume": centred(seeds[0], (C1, NX, NY, NZ), 1.0, 6.0, ((1, 2), (2, 8), (3, 16))),
        "weight_a": centred(seeds[1], (3, 3, 3, C1, C2), (27 * C1) ** -0.5, 0.21875),
        "bias_a": centred(seeds[2], (C2,), 0.5, 3.0, (), jnp.float32),
        "weight_b": centred(seeds[3], (3, 3, 3, C2, C3), (27 * C2) ** -0.5, 0.15625),
        "bias_b": centred(seeds[4], (C3,), 0.5, 3.0, (), jnp.float32),
        "cotangent": centred(seeds[5], (C3, NX // 2, NY // 2, NZ // 2), 4.0, 24.0, ((1, 32), (2, 8))),
    }


def activate(value):
    return value * jax.nn.sigmoid(value)

def slope_of(value):
    sigma = jax.nn.sigmoid(value)
    return sigma + value * sigma * (1.0 - sigma)

def conv_valid(padded, weight):
    result = lax.conv_general_dilated(padded[None], weight, (1, 1, 1), 'VALID', dimension_numbers=('NCDHW', 'DHWIO', 'NCDHW'), preferred_element_type=jnp.float32)
    return result[0]

def flipped(weight):
    return jnp.transpose(weight[::-1, ::-1, ::-1], (0, 1, 2, 4, 3))

def pad_all(field):
    return jnp.pad(field, ((0, 0), (1, 1), (1, 1), (1, 1)))

def average_pool(field):
    shape = field.shape
    split = field.reshape(shape[0], shape[1] // 2, 2, shape[2] // 2, 2, shape[3] // 2, 2)
    return lax.optimization_barrier(jnp.sum(split, axis=(2, 4, 6))) * 0.125

def spread_back(field):
    shape = field.shape
    larger = jnp.broadcast_to(field[:, :, None, :, None, :, None], (shape[0], shape[1], 2, shape[2], 2, shape[3], 2))
    return larger.reshape(shape[0], 2 * shape[1], 2 * shape[2], 2 * shape[3])

def weight_terms(padded, grad):
    width_in = padded.shape[0]
    width_out = grad.shape[0]
    extent = grad.shape[1:]
    flattened = grad.reshape(width_out, extent[0] * extent[1] * extent[2])
    products = []
    for first in range(3):
        for second in range(3):
            for third in range(3):
                window = padded[:, first:first + extent[0], second:second + extent[1], third:third + extent[2]]
                window = window.reshape(width_in, extent[0] * extent[1] * extent[2])
                products.append(lax.dot_general(window, flattened, (((1,), (1,)), ((), ())), preferred_element_type=jnp.float32))
    return jnp.stack(products).reshape(3, 3, 3, width_in, width_out)

def reference(volume, weight_a, bias_a, weight_b, bias_b, cotangent):
    scale_a = 1.0 / math.sqrt(NX * NY * NZ)
    scale_b = 1.0 / math.sqrt(NX * NY * NZ // 8)
    padded_a = pad_all(volume)
    before_a = conv_valid(padded_a, weight_a) + bias_a[:, None, None, None]
    pooled = average_pool(activate(before_a)).astype(jnp.bfloat16)
    padded_b = pad_all(pooled)
    before_b = conv_valid(padded_b, weight_b) + bias_b[:, None, None, None]
    features = activate(before_b).astype(jnp.bfloat16)
    grad_b = (cotangent.astype(jnp.float32) * slope_of(before_b)).astype(jnp.bfloat16)
    grad_weight_b = weight_terms(padded_b, grad_b) * scale_b
    grad_bias_b = lax.optimization_barrier(jnp.sum(grad_b.astype(jnp.float32), axis=(1, 2, 3))) * scale_b
    grad_pooled = conv_valid(pad_all(grad_b), flipped(weight_b)).astype(jnp.bfloat16)
    grad_a = (spread_back(grad_pooled.astype(jnp.float32)) * 0.125 * slope_of(before_a)).astype(jnp.bfloat16)
    grad_weight_a = weight_terms(padded_a, grad_a) * scale_a
    grad_bias_a = lax.optimization_barrier(jnp.sum(grad_a.astype(jnp.float32), axis=(1, 2, 3))) * scale_a
    grad_input = conv_valid(pad_all(grad_a), flipped(weight_a)).astype(jnp.bfloat16)
    return (features, grad_input, grad_weight_a, grad_bias_a, grad_weight_b, grad_bias_b)
```

```python
import math

import jax
import jax.numpy as jnp
from jax import lax
from jax.sharding import Mesh
from jax.sharding import PartitionSpec as P

GX_GY_GZ = ("gx", "gy", "gz_0", "gz_1")
GZ = ("gz_0", "gz_1")
GX_GZ = ("gx", "gz_0", "gz_1")


def padded_2(block, sides, width):
    for axis, dim in sides:
        count = lax.axis_size(axis)
        forward = [(i, i + 1) for i in range(count - 1)]
        backward = [(target, source) for source, target in forward]
        low = lax.ppermute(
            lax.slice_in_dim(block, block.shape[dim] - width, None, axis=dim), axis, forward
        )
        high = lax.ppermute(lax.slice_in_dim(block, 0, width, axis=dim), axis, backward)
        block = jnp.concatenate([low, block, high], axis=dim)
    return block


def cut_along(array, dim, length):
    lengths = array.shape
    pieces = array.reshape(*lengths[:dim], length, lengths[dim] // length, *lengths[dim + 1 :])
    return jnp.moveaxis(pieces, dim, 0)


def laid_out(pieces, dim):
    lengths = list(pieces.shape[1:])
    lengths[dim] *= pieces.shape[0]
    return jnp.moveaxis(pieces, 0, dim).reshape(lengths)


def moved_by_axis(pieces, axes, order):
    inside = pieces.shape[1:]
    result = pieces.reshape(*(lax.axis_size(a) for a in axes), *inside)
    for k in order:
        result = lax.all_to_all(result, axes[k], k, k, tiled=True)
    return result.reshape(-1, *inside)


def exchange_by_axis(array, axes, order, split_dim, concat_dim):
    pieces = cut_along(array, split_dim, lax.axis_size(axes))
    return laid_out(moved_by_axis(pieces, axes, order), concat_dim)


def together(arrays, axis):
    ends = [0]
    for a in arrays:
        ends.append(ends[-1] + a.size)
    count = lax.axis_size(axis)
    width = 640
    flat = jnp.concatenate([a.ravel().astype(jnp.bfloat16) for a in arrays])
    flat = jnp.pad(flat, (0, count * 2 * width - flat.size))
    shares = lax.all_to_all(flat.reshape(count, 2, width), axis, 0, 0, tiled=True)
    share = jnp.sum(shares.astype(jnp.float32), axis=0).astype(jnp.bfloat16)
    spread = jnp.broadcast_to(share[None], (count, 2, width))
    total = lax.all_to_all(spread, axis, 0, 0, tiled=True).ravel().astype(jnp.float32)
    return tuple((total[b:e].reshape(a.shape) for a, b, e in zip(arrays, ends, ends[1:])))


def activate(value):
    return value * jax.nn.sigmoid(value)


def slope_of(value):
    sigma = jax.nn.sigmoid(value)
    return sigma + value * sigma * (1.0 - sigma)


def conv_valid(padded, weight):
    result = lax.conv_general_dilated(
        padded[None],
        weight,
        (1, 1, 1),
        "VALID",
        dimension_numbers=("NCDHW", "DHWIO", "NCDHW"),
        preferred_element_type=jnp.float32,
    )
    return result[0]


def flipped(weight):
    return jnp.transpose(weight[::-1, ::-1, ::-1], (0, 1, 2, 4, 3))


def average_pool(field):
    shape = field.shape
    split = field.reshape(shape[0], shape[1] // 2, 2, shape[2] // 2, 2, shape[3] // 2, 2)
    return jnp.sum(split, axis=(2, 4, 6)) * 0.125


def spread_back(field):
    shape = field.shape
    larger = jnp.broadcast_to(
        field[:, :, None, :, None, :, None], (shape[0], shape[1], 2, shape[2], 2, shape[3], 2)
    )
    return larger.reshape(shape[0], 2 * shape[1], 2 * shape[2], 2 * shape[3])


def weight_terms(padded, grad):
    result = lax.conv_general_dilated(
        padded[None],
        grad[None],
        (1, 1, 1),
        "VALID",
        dimension_numbers=("CNDHW", "IODHW", "NCDHW"),
        preferred_element_type=jnp.float32,
    )
    return jnp.transpose(result, (2, 3, 4, 0, 1))


def fine_halo(field):
    return padded_2(field, (("gx", 1), ("gy", 2), (GZ, 3)), 1)


def coarse_halo(field):
    return padded_2(field, (("gx", 1), ("gy", 2), (GZ, 3)), 1)


def on_device(volume, weight_a, bias_a, weight_b, bias_b, cotangent):
    devices_all = lax.axis_size("gx") * lax.axis_size("gy") * lax.axis_size(GZ)
    cells_fine = volume.shape[1] * volume.shape[2] * volume.shape[3] * devices_all
    scale_a = 1.0 / math.sqrt(cells_fine)
    scale_b = 1.0 / math.sqrt(cells_fine // 8)
    padded_a = fine_halo(volume)
    before_a = conv_valid(padded_a, weight_a) + bias_a[:, None, None, None]
    pooled = average_pool(activate(before_a)).astype(jnp.bfloat16)
    padded_b = coarse_halo(pooled)
    before_b = conv_valid(padded_b, weight_b) + bias_b[:, None, None, None]
    features_block = activate(before_b).astype(jnp.bfloat16)
    features = exchange_by_axis(features_block, GZ, (1, 0), 1, 3)
    cotangent_block = lax.all_to_all(cotangent, GZ, split_axis=3, concat_axis=1, tiled=True)
    grad_b = (cotangent_block * slope_of(before_b)).astype(jnp.bfloat16)
    grad_pooled = conv_valid(coarse_halo(grad_b), flipped(weight_b)).astype(jnp.bfloat16)
    partial_wb = weight_terms(padded_b, grad_b)
    partial_bb = jnp.sum(grad_b, axis=(1, 2, 3), dtype=jnp.float32)
    grad_a = (spread_back(grad_pooled) * 0.125 * slope_of(before_a)).astype(jnp.bfloat16)
    partial_wa = weight_terms(padded_a, grad_a)
    partial_ba = jnp.sum(grad_a, axis=(1, 2, 3), dtype=jnp.float32)
    grad_input = conv_valid(fine_halo(grad_a), flipped(weight_a)).astype(jnp.bfloat16)
    summed_wa, summed_ba, summed_wb, summed_bb = together(
        (partial_wa, partial_ba, partial_wb, partial_bb), GX_GY_GZ
    )
    return (
        features,
        grad_input,
        summed_wa * scale_a,
        summed_ba * scale_a,
        summed_wb * scale_b,
        summed_bb * scale_b,
    )


def solution(mesh):
    finer = Mesh(
        mesh.devices.reshape(mesh.shape["gx"], mesh.shape["gy"], 8, 2), ("gx", "gy", "gz_0", "gz_1")
    )
    return jax.shard_map(
        on_device,
        mesh=finer,
        in_specs=(P(None, "gx", "gy", GZ), P(), P(), P(), P(), P(None, GX_GZ, "gy", None)),
        out_specs=(P(None, GX_GZ, "gy", None), P(None, "gx", "gy", GZ), P(), P(), P(), P()),
        check_vma=False,
    )
```

```python
import math

import jax
import jax.numpy as jnp
from jax import lax
from jax.experimental import pallas as pl
from jax.experimental.pallas import tpu as pltpu
from jax.sharding import Mesh
from jax.sharding import PartitionSpec as P

ALL = ("gx", "gy", "gz_0", "gz_1")
GZ = ("gz_0", "gz_1")
GX_GZ = ("gx", "gz_0", "gz_1")
BF16 = jnp.bfloat16
F32 = jnp.float32
TAPS = [(dx, dy) for dx in range(3) for dy in range(3)]


def call(body, outs, scratch, *args, flops=10**8):
    vmem = pl.BlockSpec(memory_space=pltpu.VMEM)
    smem = pl.BlockSpec(memory_space=pltpu.SMEM)
    return pl.pallas_call(
        body,
        out_shape=outs,
        in_specs=[smem if a.dtype == jnp.int32 else vmem for a in args],
        out_specs=jax.tree.map(lambda _: vmem, outs),
        scratch_shapes=scratch,
        compiler_params=pltpu.CompilerParams(vmem_limit_bytes=60 * 2**20),
        cost_estimate=pl.CostEstimate(flops=flops, bytes_accessed=10**6, transcendentals=0),
    )(*args)


def sds(*shape, dtype=BF16):
    return jax.ShapeDtypeStruct(shape, dtype)


def blocks(wa_ref, wb_ref):
    low = lax.broadcasted_iota(jnp.int32, (32, 128), 1) < 64
    zero_a = jnp.zeros((32, 128), BF16)
    zero_b = jnp.zeros((64, 128), BF16)

    def wa(dx, dy, dz):
        return wa_ref[(dx * 3 + dy) * 3 + dz] if 0 <= dz <= 2 else zero_a

    def wb(dx, dy, dz):
        return wb_ref[(dx * 3 + dy) * 3 + dz] if 0 <= dz <= 2 else zero_b

    def pair(first, second):
        return jnp.where(low, first.astype(F32), second.astype(F32)).astype(BF16)

    return wa, wb, pair, zero_b


def banded_ahead(wa_ref, wb_ref, a_ref, b_ref):
    wa, wb, pair, _ = blocks(wa_ref, wb_ref)
    for t, (dx, dy) in enumerate(TAPS):
        for zi in range(8):
            for p in range(2):
                a_ref[t * 256 + zi * 32 : t * 256 + zi * 32 + 32, p * 128 : p * 128 + 128] = pair(
                    wa(dx, dy, zi - 2 * p - 1), wa(dx, dy, zi - 2 * p - 2)
                )
        for zi in range(4):
            for zo in range(2):
                b_ref[t * 256 + zi * 64 : t * 256 + zi * 64 + 64, zo * 128 : zo * 128 + 128] = wb(dx, dy, zi - zo)


def banded_back(wa_ref, wb_ref, bt_ref, at_ref):
    wa, wb, pair, zero_b = blocks(wa_ref, wb_ref)
    for t, (dx, dy) in enumerate(TAPS):
        for z in range(4):
            for zi in range(4):
                dz = zi - z // 2
                block = wb(2 - dx, 2 - dy, 2 - dz) if 0 <= dz <= 2 else zero_b
                bt_ref[z * 64 : z * 64 + 64, t * 512 + zi * 128 : t * 512 + zi * 128 + 128] = block
        for z in range(8):
            for p in range(6):
                dz = 2 * p - z - 1
                at_ref[z * 32 : z * 32 + 32, t * 768 + p * 128 : t * 768 + p * 128 + 128] = pair(
                    wa(2 - dx, 2 - dy, 2 - dz), wa(2 - dx, 2 - dy, 1 - dz)
                )


def position(where_ref):
    code = where_ref[0]
    return code // 128, (code // 16) % 8, code % 16


def iota(shape, dim):
    return lax.broadcasted_iota(jnp.int32, shape, dim)


def sigmoid_of(value):
    return 0.5 * jnp.tanh(0.5 * value) + 0.5


def forward(
    where_ref, v_ref, ylo_ref, yhi_ref, zlo_ref, zhi_ref, a_ref, bias_a_ref, b_ref, bias_b_ref, cot_ref,
    feat_ref, grad_ref, sum_ref, px_ref, vo_ref, slope_ref,
    f_ref, vx_ref, s_ref, p_ref,
):
    gx, gy, gz = position(where_ref)

    def stage(src, rows, y0, q0, nq):
        def step(y, carry):
            f_ref[0:nq, 0:40, :] = src[y].astype(F32)
            for dx in range(3):
                vx_ref[dx, y0 + y, q0 : q0 + nq] = f_ref[0:nq, pl.ds(dx, 48), :].astype(BF16)

            @pl.when(jnp.logical_and(y0 + y >= 2, y0 + y < 12))
            def _():
                for dx in range(3):
                    vo_ref[dx, y0 + y - 2, q0 : q0 + nq] = f_ref[0:nq, pl.ds(dx + 2, 32), :].astype(BF16)

            return carry

        lax.fori_loop(0, rows, step, 0)

    stage(ylo_ref, 3, 0, 1, 4)
    stage(v_ref, 8, 3, 1, 4)
    stage(yhi_ref, 3, 11, 1, 4)
    stage(zlo_ref, 14, 0, 0, 1)
    stage(zhi_ref, 14, 0, 5, 1)

    fold = iota((6, 48, 128), 2) < 64
    shape = (6, 24, 128)
    x = iota(shape, 1) + (gx * 16 - 1)
    y = iota(shape, 0) + (gy * 4 - 1)
    zlane = iota(shape, 2) // 64
    inside_xy = (x >= 0) & (x < 32) & (y >= 0) & (y < 32)

    def conv_a(q, carry):
        parts = []
        for dx, dy in TAPS:
            parts.append(vx_ref[dx, dy : dy + 12, q])
            parts.append(vx_ref[dx, dy : dy + 12, q + 1])
        lhs = jnp.concatenate(parts, axis=-1).reshape(576, 2304)
        before = jnp.dot(lhs, a_ref[...], preferred_element_type=F32) + bias_a_ref[...]
        s = sigmoid_of(before)
        slope_ref[q] = (0.125 * (s * (1.0 + before * (1.0 - s)))).astype(BF16).reshape(12, 48, 256)
        act = (before * s).reshape(6, 2, 48, 256)
        rows = act[:, 0] + act[:, 1]
        lo, hi = rows[..., :128], rows[..., 128:]
        lo = lo + pltpu.roll(lo, 64, 2)
        hi = hi + pltpu.roll(hi, 64, 2)
        s_ref[...] = jnp.where(fold, lo, hi)
        mean = (s_ref[:, pl.ds(0, 24, stride=2), :] + s_ref[:, pl.ds(1, 24, stride=2), :]) * 0.125
        z = zlane + (gz * 8 - 1 + 2 * q)
        p_ref[...] = jnp.where(inside_xy & (z >= 0) & (z < 128), mean, 0.0)
        for dx in range(3):
            px_ref[dx, :, q] = p_ref[:, pl.ds(dx, 16), :].astype(BF16)
        return carry

    lax.fori_loop(0, 5, conv_a, 0)

    parts = []
    for dx, dy in TAPS:
        parts.append(px_ref[dx, dy : dy + 4, 0:4])
        parts.append(px_ref[dx, dy : dy + 4, 1:5])
    lhs = jnp.concatenate(parts, axis=-1).reshape(256, 2304)
    before = jnp.dot(lhs, b_ref[...], preferred_element_type=F32) + bias_b_ref[...]
    s = sigmoid_of(before)
    feat_ref[...] = (before * s).astype(BF16).reshape(4, 4, 16, 256)
    cot = cot_ref[...].reshape(256, 256).astype(F32)
    grad = (cot * (s * (1.0 + before * (1.0 - s)))).astype(BF16)
    grad_ref[...] = grad.reshape(4, 4, 16, 256)
    total = jnp.sum(grad.astype(F32), axis=0, keepdims=True)
    sum_ref[...] = total[:, :128] + total[:, 128:]


TN = (((0,), (0,)), ((), ()))
NT = (((1,), (1,)), ((), ()))


def weight_b_terms(px_ref, grad_ref, out_ref):
    grad = grad_ref[...].reshape(256, 256)
    for t, (dx, dy) in enumerate(TAPS):
        cells = jnp.concatenate([px_ref[dx, dy : dy + 4, 0:4], px_ref[dx, dy : dy + 4, 1:5]], axis=-1)
        terms = lax.dot_general(cells.reshape(256, 256), grad, TN, preferred_element_type=F32)
        for dz in range(3):
            out_ref[3 * t + dz] = (
                terms[dz * 64 : dz * 64 + 64, :128] + terms[dz * 64 + 64 : dz * 64 + 128, 128:]
            ).astype(BF16)


def backward(
    where_ref, g_ref, ylo_ref, yhi_ref, zlo_ref, zhi_ref, bt_ref, slope_ref, vo_ref, wb_ref, sum_b_ref,
    ga_ref, flat_ref,
    f_ref, gx_ref, s_ref, t_ref, own_ref,
):
    gx, gy, gz = position(where_ref)

    def stage(src, rows, y0, q0, nq):
        def step(y, carry):
            for h in range(2):
                f_ref[h, 0:nq, 0:24, :] = src[y, :, :, h * 128 : h * 128 + 128].astype(F32)
                for dx in range(3):
                    gx_ref[dx, y0 + y, q0 : q0 + nq, :, h * 128 : h * 128 + 128] = f_ref[
                        h, 0:nq, pl.ds(dx, 32), :
                    ].astype(BF16)
            return carry

        lax.fori_loop(0, rows, step, 0)

    stage(ylo_ref, 2, 0, 1, 4)
    stage(g_ref, 4, 2, 1, 4)
    stage(yhi_ref, 2, 6, 1, 4)
    stage(zlo_ref, 8, 0, 0, 1)
    stage(zhi_ref, 8, 0, 5, 1)

    shape = (12, 48, 128)
    x = iota(shape, 1) + (gx * 32 - 2)
    y = iota(shape, 0) + (gy * 8 - 2)
    zlane = iota(shape, 2) // 64
    inside_xy = (x >= 0) & (x < 64) & (y >= 0) & (y < 64)

    def conv_b(q, total):
        parts = []
        for dx, dy in TAPS:
            parts.append(gx_ref[dx, dy : dy + 6, q])
            parts.append(gx_ref[dx, dy : dy + 6, q + 1])
        lhs = jnp.concatenate(parts, axis=-1).reshape(192, 4608)
        pooled = lax.dot_general(lhs, bt_ref[...], NT, preferred_element_type=F32)
        pooled = pooled.astype(BF16).astype(F32).reshape(6, 32, 256)[:, :24]
        sums = []
        for h in range(2):
            half = pooled[..., h * 128 : h * 128 + 128]
            s_ref[:, pl.ds(0, 24, stride=2), :] = half
            s_ref[:, pl.ds(1, 24, stride=2), :] = half
            spread = jnp.broadcast_to(s_ref[...].reshape(6, 1, 48, 128), (6, 2, 48, 128)).reshape(12, 48, 128)
            z = zlane + (gz * 16 - 2 + 4 * q + 2 * h)
            slope = slope_ref[q, :, :, h * 128 : h * 128 + 128].astype(F32)
            t_ref[...] = jnp.where(inside_xy & (z >= 0) & (z < 256), spread * slope, 0.0)
            for dx in range(3):
                ga_ref[dx, :, q, :, h * 128 : h * 128 + 128] = t_ref[1:11, pl.ds(dx + 1, 32), :].astype(BF16)
            keep = jnp.where(q == 4 * h, 0.0, 1.0)
            own = (t_ref[2:10, pl.ds(2, 32), :] * keep).astype(BF16)
            own_ref[:, q, :, h * 128 : h * 128 + 128] = own
            sums.append(jnp.sum(own.astype(F32).reshape(256, 128), axis=0, keepdims=True))
        return total + sums[0] + sums[1]

    total = lax.fori_loop(0, 5, conv_b, jnp.zeros((1, 128), F32))
    flat_ref[0:1728] = wb_ref[...].reshape(1728, 128)
    row = iota((16, 128), 0)
    sums = jnp.where(row == 0, sum_b_ref[...], jnp.where(row == 1, total + pltpu.roll(total, 64, 1), 0.0))
    flat_ref[2304:2320] = sums.astype(BF16)
    flat_ref[2320:2560] = jnp.zeros((240, 128), BF16)

    flat = own_ref[...].reshape(1280, 256).T
    for t, (dx, dy) in enumerate(TAPS):
        cells = jnp.concatenate([vo_ref[dx, dy : dy + 8, 0:5], vo_ref[dx, dy : dy + 8, 1:6]], axis=-1)
        terms = jnp.dot(flat, cells.reshape(1280, 256), preferred_element_type=F32)
        block = terms[0:64]
        for zo in range(1, 4):
            block = block + pltpu.roll(terms[zo * 64 : zo * 64 + 64], 256 - 32 * zo, 1)
        flat_ref[1728 + 64 * t : 1792 + 64 * t] = block[:, :128].astype(BF16)


def input_grad(ga_ref, at_ref, out_ref):
    for h in range(2):
        parts = []
        for dx, dy in TAPS:
            for j in range(3):
                parts.append(ga_ref[dx, dy : dy + 8, 2 * h + j])
        lhs = jnp.concatenate(parts, axis=-1).reshape(256, 6912)
        value = lax.dot_general(lhs, at_ref[...], NT, preferred_element_type=F32)
        out_ref[:, h] = value.astype(BF16).reshape(8, 32, 256)


def ends(axis):
    count = lax.axis_size(axis)
    up = [(i, i + 1) for i in range(count - 1)]
    return up, [(b, a) for a, b in up]


def swap_sides(block, width, rows):
    first = lax.axis_index("gx") == 0
    length = block.shape[2]
    face = jnp.where(first, block[:, :, length - width :], block[:, :, :width])
    got = lax.ppermute(face, "gx", [(0, 1), (1, 0)])
    none = jnp.zeros_like(got)
    rest = jnp.zeros(block.shape[:2] + (rows - length - 2 * width,) + block.shape[3:], block.dtype)
    return jnp.concatenate([jnp.where(first, none, got), block, jnp.where(first, got, none), rest], axis=2)


def halo(block, width, x_rows):
    wide = swap_sides(block, width, x_rows)
    up, down = ends("gy")
    ylo = lax.ppermute(wide[wide.shape[0] - width :], "gy", up)
    yhi = lax.ppermute(wide[:width], "gy", down)
    up, down = ends(GZ)
    last = jnp.concatenate([ylo[:, 3:], wide[:, 3:], yhi[:, 3:]], axis=0)
    head = jnp.concatenate([ylo[:, :1], wide[:, :1], yhi[:, :1]], axis=0)
    zlo = lax.ppermute(last, GZ, up)
    zhi = lax.ppermute(head, GZ, down)
    return wide, ylo, yhi, zlo, zhi


def on_device(volume, weight_a, bias_a, weight_b, bias_b, cotangent):
    cells_fine = 64 * 64 * 256
    scale_a = 1.0 / math.sqrt(cells_fine)
    scale_b = 1.0 / math.sqrt(cells_fine // 8)
    where = lax.axis_index(ALL).astype(jnp.int32).reshape(1)

    v = jnp.transpose(volume.reshape(32, 32, 8, 4, 4), (2, 3, 1, 4, 0)).reshape(8, 4, 32, 128)
    sides = halo(v, 3, 40)

    cot = jnp.transpose(cotangent[:, 0], (2, 1, 0)).reshape(16, 8, 4, 128)
    cot = lax.all_to_all(cot, GZ, 0, 0, tiled=True)
    cot = jnp.transpose(cot.reshape(16, 4, 2, 4, 128), (3, 1, 0, 2, 4)).reshape(4, 4, 16, 256)

    wa27 = weight_a.reshape(27, 32, 64)
    wa27 = jnp.concatenate([wa27, wa27], axis=-1)
    wb27 = weight_b.reshape(27, 64, 128)
    m_a, m_b = call(banded_ahead, (sds(2304, 256), sds(2304, 256)), [], wa27, wb27, flops=10**7)
    m_bt, m_at = call(banded_back, (sds(256, 4608), sds(256, 6912)), [], wa27, wb27, flops=10**7)

    feat, grad_b, sum_b, px, vo, slope = call(
        forward,
        (
            sds(4, 4, 16, 256), sds(4, 4, 16, 256), sds(1, 128, dtype=F32),
            sds(3, 6, 5, 16, 128), sds(3, 10, 6, 32, 128), sds(5, 12, 48, 256),
        ),
        [
            pltpu.VMEM((4, 56, 128), F32), pltpu.VMEM((3, 14, 6, 48, 128), BF16),
            pltpu.VMEM((6, 48, 128), F32), pltpu.VMEM((6, 24, 128), F32),
        ],
        where, *sides, m_a, jnp.tile(bias_a, 4).reshape(1, 256), m_b, jnp.tile(bias_b, 2).reshape(1, 256), cot,
        flops=2 * 10**9,
    )

    sides_b = halo(grad_b, 2, 24)
    wb = call(weight_b_terms, sds(27, 64, 128), [], px, grad_b, flops=10**9)

    out = jnp.transpose(feat.reshape(4, 4, 16, 2, 128), (2, 1, 3, 0, 4)).reshape(16, 8, 4, 128)
    out = lax.all_to_all(out, GZ, 0, 0, tiled=True).reshape(128, 4, 128)

    ga, flat = call(
        backward,
        (sds(3, 10, 5, 32, 256), sds(2560, 128)),
        [
            pltpu.VMEM((2, 4, 40, 128), F32), pltpu.VMEM((3, 8, 6, 32, 256), BF16),
            pltpu.VMEM((6, 48, 128), F32), pltpu.VMEM((12, 48, 128), F32), pltpu.VMEM((8, 5, 32, 256), BF16),
        ],
        where, *sides_b, m_bt, slope, vo, wb, sum_b, flops=2 * 10**9,
    )

    shares = lax.all_to_all(flat.reshape(256, 5, 2, 128), ALL, 0, 0, tiled=True)
    share = jnp.sum(shares.astype(F32), axis=0).astype(BF16)
    share, out = lax.optimization_barrier((share, out))
    spread = jnp.broadcast_to(share[None], (256, 5, 2, 128))
    total = lax.all_to_all(spread, ALL, 0, 0, tiled=True).reshape(2560, 128).astype(F32)
    features = jnp.transpose(out, (2, 1, 0)).reshape(128, 1, 4, 128)

    gi = call(input_grad, sds(8, 2, 32, 256), [], ga, m_at, flops=2 * 10**9)
    gi = jnp.transpose(gi.reshape(8, 2, 32, 8, 32), (4, 2, 0, 1, 3)).reshape(32, 32, 8, 16)

    total_wb = total[:1728].reshape(3, 3, 3, 64, 128) * scale_b
    total_wa = jnp.transpose(total[1728:2304].reshape(9, 64, 4, 32)[:, :, 1:], (0, 2, 3, 1)) * scale_a
    return (
        features,
        gi,
        total_wa.reshape(3, 3, 3, 32, 64),
        total[2305, :64] * scale_a,
        total_wb,
        total[2304] * scale_b,
    )


def solution(mesh):
    finer = Mesh(
        mesh.devices.reshape(mesh.shape["gx"], mesh.shape["gy"], 8, 2), ("gx", "gy", "gz_0", "gz_1")
    )
    return jax.shard_map(
        on_device,
        mesh=finer,
        in_specs=(P(None, "gx", "gy", GZ), P(), P(), P(), P(), P(None, GX_GZ, "gy", None)),
        out_specs=(P(None, GX_GZ, "gy", None), P(None, "gx", "gy", GZ), P(), P(), P(), P()),
        check_vma=False,
    )
```

```python
import functools
import math

import jax
import jax.numpy as jnp
from jax import lax
from jax.experimental import pallas as pl
from jax.experimental.pallas import tpu as pltpu
from jax.sharding import Mesh
from jax.sharding import PartitionSpec as P

ALL = ("gx", "gy", "gz_0", "gz_1")
GZ = ("gz_0", "gz_1")
GX_GZ = ("gx", "gz_0", "gz_1")
BF16 = jnp.bfloat16
F32 = jnp.float32
TAPS = [(dx, dy) for dx in range(3) for dy in range(3)]


def call(body, outs, scratch, *args, flops=10**8):
    vmem = pl.BlockSpec(memory_space=pltpu.VMEM)
    smem = pl.BlockSpec(memory_space=pltpu.SMEM)
    return pl.pallas_call(
        body,
        out_shape=outs,
        in_specs=[smem if a.dtype == jnp.int32 else vmem for a in args],
        out_specs=jax.tree.map(lambda _: vmem, outs),
        scratch_shapes=scratch,
        compiler_params=pltpu.CompilerParams(vmem_limit_bytes=24 * 2**20),
        cost_estimate=pl.CostEstimate(flops=flops, bytes_accessed=10**6, transcendentals=0),
    )(*args)


def sds(*shape, dtype=BF16):
    return jax.ShapeDtypeStruct(shape, dtype)


def blocks(wa_ref, wb_ref):
    low = lax.broadcasted_iota(jnp.int32, (32, 128), 1) < 64
    zero_a = jnp.zeros((32, 128), BF16)
    zero_b = jnp.zeros((64, 128), BF16)

    def wa(dx, dy, dz):
        return wa_ref[(dx * 3 + dy) * 3 + dz] if 0 <= dz <= 2 else zero_a

    def wb(dx, dy, dz):
        return wb_ref[(dx * 3 + dy) * 3 + dz] if 0 <= dz <= 2 else zero_b

    def pair(first, second):
        return jnp.where(low, first.astype(F32), second.astype(F32)).astype(BF16)

    return wa, wb, pair, zero_b


def banded_ahead(wa_ref, wb_ref, a_ref, b_ref):
    wa, wb, pair, _ = blocks(wa_ref, wb_ref)
    for t, (dx, dy) in enumerate(TAPS):
        for zi in range(8):
            for p in range(2):
                a_ref[t * 256 + zi * 32 : t * 256 + zi * 32 + 32, p * 128 : p * 128 + 128] = pair(
                    wa(dx, dy, zi - 2 * p - 1), wa(dx, dy, zi - 2 * p - 2)
                )
        for zi in range(4):
            for zo in range(2):
                b_ref[t * 256 + zi * 64 : t * 256 + zi * 64 + 64, zo * 128 : zo * 128 + 128] = wb(dx, dy, zi - zo)


def banded_back_b(wb_ref, bt_ref):
    _, wb, _, zero_b = blocks(None, wb_ref)
    for t, (dx, dy) in enumerate(TAPS):
        for z in range(4):
            for zi in range(4):
                dz = zi - z // 2
                block = wb(2 - dx, 2 - dy, 2 - dz) if 0 <= dz <= 2 else zero_b
                bt_ref[z * 64 : z * 64 + 64, t * 512 + zi * 128 : t * 512 + zi * 128 + 128] = block


def banded_back_a(wa_ref, at_ref):
    wa, _, pair, _ = blocks(wa_ref, None)
    for t, (dx, dy) in enumerate(TAPS):
        for z in range(8):
            for p in range(6):
                dz = 2 * p - z - 1
                at_ref[z * 32 : z * 32 + 32, t * 768 + p * 128 : t * 768 + p * 128 + 128] = pair(
                    wa(2 - dx, 2 - dy, 2 - dz), wa(2 - dx, 2 - dy, 1 - dz)
                )


def position(where_ref):
    code = where_ref[0]
    return code // 128, (code // 16) % 8, code % 16


def iota(shape, dim):
    return lax.broadcasted_iota(jnp.int32, shape, dim)


def sigmoid_of(value):
    return 0.5 * jnp.tanh(0.5 * value) + 0.5


def forward(
    where_ref, v_ref, ynear_ref, yfar_ref, znear_ref, zfar_ref, a_ref, bias_a_ref, b_ref, bias_b_ref, cot_ref,
    feat_ref, grad_ref, sum_ref, px_ref, vo_ref, slope_ref, face_ref,
    f_ref, vx_ref, s_ref, p_ref, g_ref,
):
    gx, gy, gz = position(where_ref)

    def stage(src, rows, y0, q0, nq):
        def step(y, carry):
            f_ref[0:nq, 0:40, :] = src[y].astype(F32)
            for dx in range(3):
                vx_ref[dx, y0 + y, pl.ds(q0, nq)] = f_ref[0:nq, pl.ds(dx, 48), :].astype(BF16)

            @pl.when(jnp.logical_and(y0 + y >= 2, y0 + y < 12))
            def _():
                for dx in range(3):
                    vo_ref[dx, y0 + y - 2, pl.ds(q0, nq)] = f_ref[0:nq, pl.ds(dx + 2, 32), :].astype(BF16)

            return carry

        lax.fori_loop(0, rows, step, 0)

    even_y, even_z = gy % 2 == 0, gz % 2 == 0
    stage(v_ref, 8, 3, 1, 4)
    stage(ynear_ref, 3, jnp.where(even_y, 11, 0), 1, 4)
    stage(yfar_ref, 3, jnp.where(even_y, 0, 11), 1, 4)
    stage(znear_ref, 14, 0, jnp.where(even_z, 5, 0), 1)
    stage(zfar_ref, 14, 0, jnp.where(even_z, 0, 5), 1)

    fold = iota((6, 48, 128), 2) < 64
    shape = (6, 24, 128)
    x = iota(shape, 1) + (gx * 16 - 1)
    y = iota(shape, 0) + (gy * 4 - 1)
    zlane = iota(shape, 2) // 64
    inside_xy = (x >= 0) & (x < 32) & (y >= 0) & (y < 32)

    def conv_a(q, carry):
        parts = []
        for dx, dy in TAPS:
            parts.append(vx_ref[dx, dy : dy + 12, q])
            parts.append(vx_ref[dx, dy : dy + 12, q + 1])
        lhs = jnp.concatenate(parts, axis=-1).reshape(576, 2304)
        before = jnp.dot(lhs, a_ref[...], preferred_element_type=F32) + bias_a_ref[...]
        s = sigmoid_of(before)
        slope_ref[q] = (0.125 * (s * (1.0 + before * (1.0 - s)))).astype(BF16).reshape(12, 48, 256)
        act = (before * s).reshape(6, 2, 48, 256)
        rows = act[:, 0] + act[:, 1]
        lo, hi = rows[..., :128], rows[..., 128:]
        lo = lo + pltpu.roll(lo, 64, 2)
        hi = hi + pltpu.roll(hi, 64, 2)
        s_ref[...] = jnp.where(fold, lo, hi)
        mean = (s_ref[:, pl.ds(0, 24, stride=2), :] + s_ref[:, pl.ds(1, 24, stride=2), :]) * 0.125
        z = zlane + (gz * 8 - 1 + 2 * q)
        p_ref[...] = jnp.where(inside_xy & (z >= 0) & (z < 128), mean, 0.0)
        for dx in range(3):
            px_ref[dx, :, q] = p_ref[:, pl.ds(dx, 16), :].astype(BF16)
        return carry

    lax.fori_loop(0, 5, conv_a, 0)

    parts = []
    for dx, dy in TAPS:
        parts.append(px_ref[dx, dy : dy + 4, 0:4])
        parts.append(px_ref[dx, dy : dy + 4, 1:5])
    lhs = jnp.concatenate(parts, axis=-1).reshape(256, 2304)
    before = jnp.dot(lhs, b_ref[...], preferred_element_type=F32) + bias_b_ref[...]
    s = sigmoid_of(before)
    feat_ref[...] = (before * s).astype(BF16).reshape(4, 4, 16, 256)
    cot = cot_ref[...].reshape(256, 256).astype(F32)
    grad = (cot * (s * (1.0 + before * (1.0 - s)))).astype(BF16)
    grad_ref[...] = grad.reshape(4, 4, 16, 256)
    wide = grad.astype(F32)
    total = jnp.sum(wide, axis=0, keepdims=True)
    sum_ref[...] = total[:, :128] + total[:, 128:]
    for h in range(2):
        lanes = slice(h * 128, h * 128 + 128)
        g_ref[...] = wide[:, lanes].reshape(4, 4, 16, 128)
        face_ref[..., lanes] = jnp.where(gx == 0, g_ref[:, :, pl.ds(14, 2), :], g_ref[:, :, pl.ds(0, 2), :]).astype(BF16)


TN = (((0,), (0,)), ((), ()))
NT = (((1,), (1,)), ((), ()))


def weight_b_terms(px_ref, grad_ref, out_ref):
    grad = grad_ref[...].reshape(256, 256)
    for t, (dx, dy) in enumerate(TAPS):
        cells = jnp.concatenate([px_ref[dx, dy : dy + 4, 0:4], px_ref[dx, dy : dy + 4, 1:5]], axis=-1)
        terms = lax.dot_general(cells.reshape(256, 256), grad, TN, preferred_element_type=F32)
        for dz in range(3):
            out_ref[3 * t + dz] = (
                terms[dz * 64 : dz * 64 + 64, :128] + terms[dz * 64 + 64 : dz * 64 + 128, 128:]
            ).astype(BF16)


def backward(
    where_ref, g_ref, ynear_ref, yfar_ref, znear_ref, zfar_ref, bt_ref, slope_ref, vo_ref, wb_ref, sum_b_ref,
    ga_ref, keep_ref, send_ref,
    f_ref, gx_ref, s_ref, t_ref, own_ref, flat_ref,
):
    gx, gy, gz = position(where_ref)

    def stage(src, rows, y0, q0, nq):
        def step(y, carry):
            for h in range(2):
                f_ref[h, 0:nq, 0:24, :] = src[y, :, :, h * 128 : h * 128 + 128].astype(F32)
                for dx in range(3):
                    gx_ref[dx, y0 + y, pl.ds(q0, nq), :, h * 128 : h * 128 + 128] = f_ref[
                        h, 0:nq, pl.ds(dx, 32), :
                    ].astype(BF16)
            return carry

        lax.fori_loop(0, rows, step, 0)

    even_y, even_z = gy % 2 == 0, gz % 2 == 0
    stage(g_ref, 4, 2, 1, 4)
    stage(ynear_ref, 2, jnp.where(even_y, 6, 0), 1, 4)
    stage(yfar_ref, 2, jnp.where(even_y, 0, 6), 1, 4)
    stage(znear_ref, 8, 0, jnp.where(even_z, 5, 0), 1)
    stage(zfar_ref, 8, 0, jnp.where(even_z, 0, 5), 1)

    shape = (12, 48, 128)
    x = iota(shape, 1) + (gx * 32 - 2)
    y = iota(shape, 0) + (gy * 8 - 2)
    zlane = iota(shape, 2) // 64
    inside_xy = (x >= 0) & (x < 64) & (y >= 0) & (y < 64)

    def conv_b(q, total):
        parts = []
        for dx, dy in TAPS:
            parts.append(gx_ref[dx, dy : dy + 6, q])
            parts.append(gx_ref[dx, dy : dy + 6, q + 1])
        lhs = jnp.concatenate(parts, axis=-1).reshape(192, 4608)
        pooled = lax.dot_general(lhs, bt_ref[...], NT, preferred_element_type=F32)
        pooled = pooled.astype(BF16).astype(F32).reshape(6, 32, 256)[:, :24]
        sums = []
        for h in range(2):
            half = pooled[..., h * 128 : h * 128 + 128]
            s_ref[:, pl.ds(0, 24, stride=2), :] = half
            s_ref[:, pl.ds(1, 24, stride=2), :] = half
            spread = jnp.broadcast_to(s_ref[...].reshape(6, 1, 48, 128), (6, 2, 48, 128)).reshape(12, 48, 128)
            z = zlane + (gz * 16 - 2 + 4 * q + 2 * h)
            slope = slope_ref[q, :, :, h * 128 : h * 128 + 128].astype(F32)
            t_ref[...] = jnp.where(inside_xy & (z >= 0) & (z < 256), spread * slope, 0.0)
            for dx in range(3):
                ga_ref[dx, :, q, :, h * 128 : h * 128 + 128] = t_ref[1:11, pl.ds(dx + 1, 32), :].astype(BF16)
            keep = jnp.where(q == 4 * h, 0.0, 1.0)
            own = (t_ref[2:10, pl.ds(2, 32), :] * keep).astype(BF16)
            own_ref[:, q, :, h * 128 : h * 128 + 128] = own
            sums.append(jnp.sum(own.astype(F32).reshape(256, 128), axis=0, keepdims=True))
        return total + sums[0] + sums[1]

    total = lax.fori_loop(0, 5, conv_b, jnp.zeros((1, 128), F32))
    flat_ref[0:1728] = wb_ref[...].reshape(1728, 128)
    row = iota((16, 128), 0)
    sums = jnp.where(row == 0, sum_b_ref[...], jnp.where(row == 1, total + pltpu.roll(total, 64, 1), 0.0))
    flat_ref[2304:2320] = sums.astype(BF16)
    flat_ref[2320:2560] = jnp.zeros((240, 128), BF16)

    flat = own_ref[...].reshape(1280, 256).T
    for t, (dx, dy) in enumerate(TAPS):
        cells = jnp.concatenate([vo_ref[dx, dy : dy + 8, 0:5], vo_ref[dx, dy : dy + 8, 1:6]], axis=-1)
        terms = jnp.dot(flat, cells.reshape(1280, 256), preferred_element_type=F32)
        block = terms[0:64]
        for zo in range(1, 4):
            block = block + pltpu.roll(terms[zo * 64 : zo * 64 + 64], 256 - 32 * zo, 1)
        flat_ref[1728 + 64 * t : 1792 + 64 * t] = block[:, :128].astype(BF16)

    half = pl.multiple_of((gz % 2) * 1280, 1280)
    rest = pl.multiple_of((1 - gz % 2) * 1280, 1280)
    keep_ref[...] = flat_ref[pl.ds(half, 1280), :]
    send_ref[...] = flat_ref[pl.ds(rest, 1280), :]


def finish(scale_a, scale_b, where_ref, mine_ref, other_ref, wa_ref, ba_ref, wb_ref, bb_ref):
    core = where_ref[0] % 2

    def put(first_ref, second_ref):
        wb_ref[0:1280] = first_ref[...].astype(F32) * scale_b
        wb_ref[1280:1728] = second_ref[0:448].astype(F32) * scale_b
        for t in range(9):
            block = second_ref[448 + 64 * t : 512 + 64 * t].astype(F32).T * scale_a
            for dz in range(3):
                wa_ref[3 * t + dz] = block[32 + 32 * dz : 64 + 32 * dz]
        tail = second_ref[1024:1040].astype(F32)
        bb_ref[...] = tail[0:1] * scale_b
        ba_ref[...] = tail[1:2, :64] * scale_a

    @pl.when(core == 0)
    def _():
        put(mine_ref, other_ref)

    @pl.when(core == 1)
    def _():
        put(other_ref, mine_ref)


def input_grad(ga_ref, at_ref, out_ref):
    for h in range(2):
        parts = []
        for dx, dy in TAPS:
            for j in range(3):
                parts.append(ga_ref[dx, dy : dy + 8, 2 * h + j])
        lhs = jnp.concatenate(parts, axis=-1).reshape(256, 6912)
        value = lax.dot_general(lhs, at_ref[...], NT, preferred_element_type=F32)
        out_ref[:, h] = value.astype(BF16).reshape(8, 32, 256)


def swaps(axis):
    count = lax.axis_size(axis)
    near = [(i, i ^ 1) for i in range(count)]
    far = [(i, i + 1 if i % 2 else i - 1) for i in range(1, count - 1)]
    return lax.axis_index(axis) % 2 == 0, near, far


def halo(block, face, width, x_rows):
    first = lax.axis_index("gx") == 0
    got = lax.ppermute(face, "gx", [(0, 1), (1, 0)])
    none = jnp.zeros_like(got)
    rest = jnp.zeros(block.shape[:2] + (x_rows - block.shape[2] - 2 * width,) + block.shape[3:], block.dtype)
    wide = jnp.concatenate([jnp.where(first, none, got), block, jnp.where(first, got, none), rest], axis=2)
    even, near, far = swaps("gy")
    low, high = wide[:width], wide[wide.shape[0] - width :]
    yfar = lax.ppermute(jnp.where(even, low, high), "gy", far)
    ynear = lax.ppermute(jnp.where(even, high, low), "gy", near)
    ylo, yhi = jnp.where(even, yfar, ynear), jnp.where(even, ynear, yfar)
    even, near, far = swaps(GZ)
    last = jnp.concatenate([ylo[:, 3:], wide[:, 3:], yhi[:, 3:]], axis=0)
    head = jnp.concatenate([ylo[:, :1], wide[:, :1], yhi[:, :1]], axis=0)
    zfar = lax.ppermute(jnp.where(even, head, last), GZ, far)
    znear = lax.ppermute(jnp.where(even, last, head), GZ, near)
    return wide, ynear, yfar, znear, zfar


CHIPS = ("gx", "gy", "gz_0")


def to_slabs(pieces):
    index = lax.axis_index(GZ)
    shape = pieces.shape
    for b in range(4):
        other = 1 - (index >> b) % 2
        pieces = pieces.reshape((16 >> (b + 1), 2, 1 << b) + shape[1:])
        part = lax.dynamic_index_in_dim(pieces, other, 1)
        got = lax.ppermute(part, GZ, [(i, i ^ (1 << b)) for i in range(16)])
        pieces = lax.dynamic_update_slice_in_dim(pieces, got, other, 1)
    return pieces.reshape(shape)


def on_device(volume, weight_a, bias_a, weight_b, bias_b, cotangent):
    cells_fine = 64 * 64 * 256
    scale_a = 1.0 / math.sqrt(cells_fine)
    scale_b = 1.0 / math.sqrt(cells_fine // 8)
    where = lax.axis_index(ALL).astype(jnp.int32).reshape(1)

    v = jnp.transpose(volume.reshape(32, 32, 8, 4, 4), (2, 3, 1, 4, 0)).reshape(8, 4, 32, 128)
    face = jnp.where(lax.axis_index("gx") == 0, v[:, :, 29:32], v[:, :, 0:3])
    sides = halo(v, face, 3, 40)

    cot = jnp.transpose(cotangent[:, 0], (2, 1, 0)).reshape(16, 8, 4, 128)
    cot = lax.all_to_all(cot, GZ, 0, 0, tiled=True)
    cot = jnp.transpose(cot.reshape(16, 4, 2, 4, 128), (3, 1, 0, 2, 4)).reshape(4, 4, 16, 256)

    wa27 = weight_a.reshape(27, 32, 64)
    wa27 = jnp.concatenate([wa27, wa27], axis=-1)
    wb27 = weight_b.reshape(27, 64, 128)
    m_a, m_b = call(banded_ahead, (sds(2304, 256), sds(2304, 256)), [], wa27, wb27, flops=10**7)
    m_bt = call(banded_back_b, sds(256, 4608), [], wb27, flops=10**7)
    m_at = call(banded_back_a, sds(256, 6912), [], wa27, flops=10**7)

    feat, grad_b, sum_b, px, vo, slope, face_b = call(
        forward,
        (
            sds(4, 4, 16, 256), sds(4, 4, 16, 256), sds(1, 128, dtype=F32),
            sds(3, 6, 5, 16, 128), sds(3, 10, 6, 32, 128), sds(5, 12, 48, 256),
            sds(4, 4, 2, 256),
        ),
        [
            pltpu.VMEM((4, 56, 128), F32), pltpu.VMEM((3, 14, 6, 48, 128), BF16),
            pltpu.VMEM((6, 48, 128), F32), pltpu.VMEM((6, 24, 128), F32), pltpu.VMEM((4, 4, 16, 128), F32),
        ],
        where, *sides, m_a, jnp.tile(bias_a, 4).reshape(1, 256), m_b, jnp.tile(bias_b, 2).reshape(1, 256), cot,
        flops=2 * 10**9,
    )

    sides_b = halo(grad_b, face_b, 2, 24)
    wb = call(weight_b_terms, sds(27, 64, 128), [], px, grad_b, flops=10**9)

    out = jnp.transpose(feat.reshape(4, 4, 16, 2, 128), (2, 1, 3, 0, 4)).reshape(16, 8, 4, 128)

    ga, keep, send = call(
        backward,
        (sds(3, 10, 5, 32, 256), sds(1280, 128), sds(1280, 128)),
        [
            pltpu.VMEM((2, 4, 40, 128), F32), pltpu.VMEM((3, 8, 6, 32, 256), BF16),
            pltpu.VMEM((6, 48, 128), F32), pltpu.VMEM((12, 48, 128), F32), pltpu.VMEM((8, 5, 32, 256), BF16),
            pltpu.VMEM((2560, 128), BF16),
        ],
        where, *sides_b, m_bt, slope, vo, wb, sum_b, flops=2 * 10**9,
    )

    flip = [(0, 1), (1, 0)]
    count = lax.axis_size(CHIPS)
    got = lax.ppermute(send, "gz_1", flip)
    chip = (keep.astype(F32) + got.astype(F32)).astype(BF16)
    shares = lax.all_to_all(chip.reshape(count, 5, 2, 128), CHIPS, 0, 0, tiled=True)
    share = jnp.sum(shares.astype(F32), axis=0).astype(BF16)
    spread = jnp.broadcast_to(share[None], (count, 5, 2, 128))
    mine = lax.all_to_all(spread, CHIPS, 0, 0, tiled=True).reshape(count * 10, 128)
    other = lax.ppermute(mine, "gz_1", flip)
    features = jnp.transpose(to_slabs(out).reshape(128, 4, 128), (2, 1, 0)).reshape(128, 1, 4, 128)

    gi = call(input_grad, sds(8, 2, 32, 256), [], ga, m_at, flops=2 * 10**9)
    gi = jnp.transpose(gi.reshape(8, 2, 32, 8, 32), (4, 2, 0, 1, 3)).reshape(32, 32, 8, 16)

    total_wa, total_ba, total_wb, total_bb = call(
        functools.partial(finish, scale_a, scale_b),
        (sds(27, 32, 64, dtype=F32), sds(1, 64, dtype=F32), sds(1728, 128, dtype=F32), sds(1, 128, dtype=F32)),
        [], where, mine, other, flops=10**6,
    )
    return (
        features,
        gi,
        total_wa.reshape(3, 3, 3, 32, 64),
        total_ba.reshape(64),
        total_wb.reshape(3, 3, 3, 64, 128),
        total_bb.reshape(128),
    )


def solution(mesh):
    finer = Mesh(
        mesh.devices.reshape(mesh.shape["gx"], mesh.shape["gy"], 8, 2), ("gx", "gy", "gz_0", "gz_1")
    )
    return jax.shard_map(
        on_device,
        mesh=finer,
        in_specs=(P(None, "gx", "gy", GZ), P(), P(), P(), P(), P(None, GX_GZ, "gy", None)),
        out_specs=(P(None, GX_GZ, "gy", None), P(None, "gx", "gy", GZ), P(), P(), P(), P()),
        check_vma=False,
    )
```

```python
import functools
import math

import jax
import jax.numpy as jnp
from jax import lax
from jax.experimental import pallas as pl
from jax.experimental.pallas import tpu as pltpu
from jax.sharding import Mesh
from jax.sharding import PartitionSpec as P

ALL = ("gx", "gy", "gz_0", "gz_1")
GZ = ("gz_0", "gz_1")
GX_GZ = ("gx", "gz_0", "gz_1")
BF16 = jnp.bfloat16
F32 = jnp.float32
TAPS = [(dx, dy) for dx in range(3) for dy in range(3)]


def call(body, outs, scratch, *args, flops=10**8, room=8, far_args=0, far_outs=0):
    vmem = pl.BlockSpec(memory_space=pltpu.VMEM)
    smem = pl.BlockSpec(memory_space=pltpu.SMEM)
    far = pl.BlockSpec(memory_space=pltpu.HBM)
    near = [smem if a.dtype == jnp.int32 else vmem for a in args[: len(args) - far_args]]
    if isinstance(outs, tuple):
        out_specs = (vmem,) * (len(outs) - far_outs) + (far,) * far_outs
    else:
        out_specs = vmem
    return pl.pallas_call(
        body,
        out_shape=outs,
        in_specs=near + [far] * far_args,
        out_specs=out_specs,
        scratch_shapes=scratch,
        compiler_params=pltpu.CompilerParams(vmem_limit_bytes=room * 2**20),
        cost_estimate=pl.CostEstimate(flops=flops, bytes_accessed=10**6, transcendentals=0),
    )(*args)


def sds(*shape, dtype=BF16):
    return jax.ShapeDtypeStruct(shape, dtype)


def doubled(w_ref, out_ref):
    w = w_ref[...].astype(F32)
    out_ref[...] = jnp.concatenate([w, w], axis=-1).astype(BF16)


def blocks(wa_ref, wb_ref):
    low = lax.broadcasted_iota(jnp.int32, (32, 128), 1) < 64
    zero_a = jnp.zeros((32, 128), BF16)
    zero_b = jnp.zeros((64, 128), BF16)

    def wa(dx, dy, dz):
        return wa_ref[(dx * 3 + dy) * 3 + dz] if 0 <= dz <= 2 else zero_a

    def wb(dx, dy, dz):
        return wb_ref[(dx * 3 + dy) * 3 + dz] if 0 <= dz <= 2 else zero_b

    def pair(first, second):
        return jnp.where(low, first.astype(F32), second.astype(F32)).astype(BF16)

    return wa, wb, pair, zero_b


def banded_ahead_a(w_ref, a_ref, double_ref):
    doubled(w_ref, double_ref)
    wa, _, pair, _ = blocks(double_ref, None)
    for t, (dx, dy) in enumerate(TAPS):
        for zi in range(8):
            for p in range(2):
                a_ref[t * 256 + zi * 32 : t * 256 + zi * 32 + 32, p * 128 : p * 128 + 128] = pair(
                    wa(dx, dy, zi - 2 * p - 1), wa(dx, dy, zi - 2 * p - 2)
                )


def banded_ahead_b(wb_ref, b_ref):
    _, wb, _, _ = blocks(None, wb_ref)
    for t, (dx, dy) in enumerate(TAPS):
        for zi in range(4):
            for zo in range(2):
                b_ref[t * 256 + zi * 64 : t * 256 + zi * 64 + 64, zo * 128 : zo * 128 + 128] = wb(dx, dy, zi - zo)


def banded_back_b(wb_ref, bt_ref):
    _, wb, _, zero_b = blocks(None, wb_ref)
    for t, (dx, dy) in enumerate(TAPS):
        for z in range(4):
            for zi in range(4):
                dz = zi - z // 2
                block = wb(2 - dx, 2 - dy, 2 - dz) if 0 <= dz <= 2 else zero_b
                bt_ref[z * 64 : z * 64 + 64, t * 512 + zi * 128 : t * 512 + zi * 128 + 128] = block


def banded_back_a(wa_ref, at_ref):
    wa, _, pair, _ = blocks(wa_ref, None)
    for t, (dx, dy) in enumerate(TAPS):
        for z in range(8):
            for p in range(6):
                dz = 2 * p - z - 1
                at_ref[z * 32 : z * 32 + 32, t * 768 + p * 128 : t * 768 + p * 128 + 128] = pair(
                    wa(2 - dx, 2 - dy, 2 - dz), wa(2 - dx, 2 - dy, 1 - dz)
                )


def position(where_ref):
    code = where_ref[0]
    return code // 128, (code // 16) % 8, code % 16


def iota(shape, dim):
    return lax.broadcasted_iota(jnp.int32, shape, dim)


def sigmoid_of(value):
    return 0.5 * jnp.tanh(0.5 * value) + 0.5


def in_rows(v_ref, out_ref, f_ref):
    for y in range(8):
        f_ref[y % 2] = v_ref[:, y].astype(F32).reshape(512, 32)
        for q in range(4):
            columns = [f_ref[y % 2, pl.ds(4 * q + z, 32, stride=16), :] for z in range(4)]
            out_ref[y, q] = jnp.concatenate(columns, axis=0).T.astype(BF16)


def forward(
    where_ref, v_ref, ynear_ref, yfar_ref, znear_ref, zfar_ref, a_ref, bias_a_ref, wb_ref, bias_b_ref, cot_ref,
    feat_ref, grad_ref, sum_ref, px_ref, face_ref, vo_hbm, slope_hbm,
    f_ref, vx_ref, s_ref, p_ref, g_ref, b_ref, vo_ref, slope_ref, sem,
):
    banded_ahead_b(wb_ref, b_ref)
    twice = jnp.concatenate([bias_a_ref[...], bias_a_ref[...]], axis=-1)
    bias_a = jnp.concatenate([twice, twice], axis=-1)
    bias_b = jnp.concatenate([bias_b_ref[...], bias_b_ref[...]], axis=-1)
    gx, gy, gz = position(where_ref)

    def stage(src, rows, y0, q0, nq):
        def step(y, carry):
            f_ref[0:nq, 0:40, :] = src[y].astype(F32)
            for dx in range(3):
                vx_ref[dx, y0 + y, pl.ds(q0, nq)] = f_ref[0:nq, pl.ds(dx, 48), :].astype(BF16)

            @pl.when(jnp.logical_and(y0 + y >= 2, y0 + y < 12))
            def _():
                vo_ref[y0 + y - 2, pl.ds(q0, nq)] = f_ref[0:nq, pl.ds(2, 40), :].astype(BF16)

            return carry

        lax.fori_loop(0, rows, step, 0)

    even_y, even_z = gy % 2 == 0, gz % 2 == 0
    stage(v_ref, 8, 3, 1, 4)
    stage(ynear_ref, 3, jnp.where(even_y, 11, 0), 1, 4)
    stage(yfar_ref, 3, jnp.where(even_y, 0, 11), 1, 4)
    stage(znear_ref, 14, 0, jnp.where(even_z, 5, 0), 1)
    stage(zfar_ref, 14, 0, jnp.where(even_z, 0, 5), 1)

    save_vo = pltpu.make_async_copy(vo_ref, vo_hbm, sem.at[5])
    save_vo.start()

    def save_slope(q):
        return pltpu.make_async_copy(slope_ref.at[q], slope_hbm.at[q], sem.at[q])

    fold = iota((6, 48, 128), 2) < 64
    shape = (6, 24, 128)
    x = iota(shape, 1) + (gx * 16 - 1)
    y = iota(shape, 0) + (gy * 4 - 1)
    zlane = iota(shape, 2) // 64
    inside_xy = (x >= 0) & (x < 32) & (y >= 0) & (y < 32)

    def conv_a(q, carry):
        parts = []
        for dx, dy in TAPS:
            parts.append(vx_ref[dx, dy : dy + 12, q])
            parts.append(vx_ref[dx, dy : dy + 12, q + 1])
        lhs = jnp.concatenate(parts, axis=-1).reshape(576, 2304)
        before = jnp.dot(lhs, a_ref[...], preferred_element_type=F32) + bias_a
        s = sigmoid_of(before)
        slope = (0.125 * (s * (1.0 + before * (1.0 - s)))).astype(BF16)
        slope_ref[q] = slope.reshape(12, 48, 256)[1:11]
        save_slope(q).start()
        act = (before * s).reshape(6, 2, 48, 256)
        rows = act[:, 0] + act[:, 1]
        lo, hi = rows[..., :128], rows[..., 128:]
        lo = lo + pltpu.roll(lo, 64, 2)
        hi = hi + pltpu.roll(hi, 64, 2)
        s_ref[...] = jnp.where(fold, lo, hi)
        mean = (s_ref[:, pl.ds(0, 24, stride=2), :] + s_ref[:, pl.ds(1, 24, stride=2), :]) * 0.125
        z = zlane + (gz * 8 - 1 + 2 * q)
        p_ref[...] = jnp.where(inside_xy & (z >= 0) & (z < 128), mean, 0.0)
        for dx in range(3):
            px_ref[dx, :, q] = p_ref[:, pl.ds(dx, 16), :].astype(BF16)
        return carry

    lax.fori_loop(0, 5, conv_a, 0)

    parts = []
    for dx, dy in TAPS:
        parts.append(px_ref[dx, dy : dy + 4, 0:4])
        parts.append(px_ref[dx, dy : dy + 4, 1:5])
    lhs = jnp.concatenate(parts, axis=-1).reshape(256, 2304)
    before = jnp.dot(lhs, b_ref[...], preferred_element_type=F32) + bias_b
    s = sigmoid_of(before)
    feat_ref[...] = (before * s).astype(BF16).reshape(4, 4, 16, 256)
    cot = cot_ref[...].reshape(256, 256).astype(F32)
    grad = (cot * (s * (1.0 + before * (1.0 - s)))).astype(BF16)
    grad_ref[...] = grad.reshape(4, 4, 16, 256)
    wide = grad.astype(F32)
    total = jnp.sum(wide, axis=0, keepdims=True)
    sum_ref[...] = total[:, :128] + total[:, 128:]
    for h in range(2):
        lanes = slice(h * 128, h * 128 + 128)
        g_ref[...] = wide[:, lanes].reshape(4, 4, 16, 128)
        face_ref[..., lanes] = jnp.where(gx == 0, g_ref[:, :, pl.ds(14, 2), :], g_ref[:, :, pl.ds(0, 2), :]).astype(BF16)
    for q in range(5):
        save_slope(q).wait()
    save_vo.wait()


TN = (((0,), (0,)), ((), ()))
NT = (((1,), (1,)), ((), ()))


def weight_b_terms(px_ref, grad_ref, out_ref):
    grad = grad_ref[...].reshape(256, 256)
    for t, (dx, dy) in enumerate(TAPS):
        cells = jnp.concatenate([px_ref[dx, dy : dy + 4, 0:4], px_ref[dx, dy : dy + 4, 1:5]], axis=-1)
        terms = lax.dot_general(cells.reshape(256, 256), grad, TN, preferred_element_type=F32)
        for dz in range(3):
            out_ref[3 * t + dz] = (
                terms[dz * 64 : dz * 64 + 64, :128] + terms[dz * 64 + 64 : dz * 64 + 128, 128:]
            ).astype(BF16)


def backward(
    where_ref, g_ref, ynear_ref, yfar_ref, znear_ref, zfar_ref, w_ref, wb_ref, sum_b_ref, slope_ref, vo_ref,
    keep_ref, send_ref, ga_hbm,
    f_ref, gx_ref, s_ref, t_ref, own_ref, flat_ref, vx_ref, v_ref, bt_ref, ga_ref, sem,
):
    banded_back_b(w_ref, bt_ref)
    gx, gy, gz = position(where_ref)

    def stage(src, rows, y0, q0, nq):
        def step(y, carry):
            for h in range(2):
                f_ref[h, 0:nq, 0:24, :] = src[y, :, :, h * 128 : h * 128 + 128].astype(F32)
                for dx in range(3):
                    gx_ref[dx, y0 + y, pl.ds(q0, nq), :, h * 128 : h * 128 + 128] = f_ref[
                        h, 0:nq, pl.ds(dx, 32), :
                    ].astype(BF16)
            return carry

        lax.fori_loop(0, rows, step, 0)

    even_y, even_z = gy % 2 == 0, gz % 2 == 0
    stage(g_ref, 4, 2, 1, 4)
    stage(ynear_ref, 2, jnp.where(even_y, 6, 0), 1, 4)
    stage(yfar_ref, 2, jnp.where(even_y, 0, 6), 1, 4)
    stage(znear_ref, 8, 0, jnp.where(even_z, 5, 0), 1)
    stage(zfar_ref, 8, 0, jnp.where(even_z, 0, 5), 1)

    def stage_v(y, carry):
        v_ref[...] = vo_ref[y].astype(F32)
        for dx in range(3):
            vx_ref[dx, y] = v_ref[:, pl.ds(dx, 32), :].astype(BF16)
        return carry

    lax.fori_loop(0, 10, stage_v, 0)

    shape = (10, 48, 128)
    x = iota(shape, 1) + (gx * 32 - 2)
    y = iota(shape, 0) + (gy * 8 - 1)
    zlane = iota(shape, 2) // 64
    inside_xy = (x >= 0) & (x < 64) & (y >= 0) & (y < 64)

    def save_ga(q):
        return pltpu.make_async_copy(ga_ref.at[q], ga_hbm.at[q], sem.at[q])

    def conv_b(q, total):
        parts = []
        for dx, dy in TAPS:
            parts.append(gx_ref[dx, dy : dy + 6, q])
            parts.append(gx_ref[dx, dy : dy + 6, q + 1])
        lhs = jnp.concatenate(parts, axis=-1).reshape(192, 4608)
        pooled = lax.dot_general(lhs, bt_ref[...], NT, preferred_element_type=F32)
        pooled = pooled.astype(BF16).astype(F32).reshape(6, 32, 256)[:, :24]
        sums = []
        for h in range(2):
            half = pooled[..., h * 128 : h * 128 + 128]
            s_ref[:, pl.ds(0, 24, stride=2), :] = half
            s_ref[:, pl.ds(1, 24, stride=2), :] = half
            spread = jnp.broadcast_to(s_ref[...].reshape(6, 1, 48, 128), (6, 2, 48, 128)).reshape(12, 48, 128)[1:11]
            z = zlane + (gz * 16 - 2 + 4 * q + 2 * h)
            slope = slope_ref[q, :, :, h * 128 : h * 128 + 128].astype(F32)
            t_ref[...] = jnp.where(inside_xy & (z >= 0) & (z < 256), spread * slope, 0.0)
            ga_ref[q, :, :, h * 128 : h * 128 + 128] = t_ref[:, pl.ds(1, 40), :].astype(BF16)
            keep = jnp.where(q == 4 * h, 0.0, 1.0)
            own = (t_ref[1:9, pl.ds(2, 32), :] * keep).astype(BF16)
            own_ref[:, q, :, h * 128 : h * 128 + 128] = own
            sums.append(jnp.sum(own.astype(F32).reshape(256, 128), axis=0, keepdims=True))
        save_ga(q).start()
        return total + sums[0] + sums[1]

    total = lax.fori_loop(0, 5, conv_b, jnp.zeros((1, 128), F32))
    flat_ref[0:1728] = wb_ref[...].reshape(1728, 128)
    row = iota((16, 128), 0)
    sums = jnp.where(row == 0, sum_b_ref[...], jnp.where(row == 1, total + pltpu.roll(total, 64, 1), 0.0))
    flat_ref[2304:2320] = sums.astype(BF16)
    flat_ref[2320:2560] = jnp.zeros((240, 128), BF16)

    flat = own_ref[...].reshape(1280, 256).T
    for t, (dx, dy) in enumerate(TAPS):
        cells = jnp.concatenate([vx_ref[dx, dy : dy + 8, 0:5], vx_ref[dx, dy : dy + 8, 1:6]], axis=-1)
        terms = jnp.dot(flat, cells.reshape(1280, 256), preferred_element_type=F32)
        block = terms[0:64]
        for zo in range(1, 4):
            block = block + pltpu.roll(terms[zo * 64 : zo * 64 + 64], 256 - 32 * zo, 1)
        flat_ref[1728 + 64 * t : 1792 + 64 * t] = block[:, :128].astype(BF16)

    half = pl.multiple_of((gz % 2) * 1280, 1280)
    rest = pl.multiple_of((1 - gz % 2) * 1280, 1280)
    keep_ref[...] = flat_ref[pl.ds(half, 1280), :]
    send_ref[...] = flat_ref[pl.ds(rest, 1280), :]
    for q in range(5):
        save_ga(q).wait()


def finish(scale_a, scale_b, where_ref, mine_ref, other_ref, wa_ref, ba_ref, wb_ref, bb_ref):
    core = where_ref[0] % 2

    def put(first_ref, second_ref):
        wb_ref[0:1280] = first_ref[...].astype(F32) * scale_b
        wb_ref[1280:1728] = second_ref[0:448].astype(F32) * scale_b
        for t in range(9):
            block = second_ref[448 + 64 * t : 512 + 64 * t].astype(F32).T * scale_a
            for dz in range(3):
                wa_ref[3 * t + dz] = block[32 + 32 * dz : 64 + 32 * dz]
        tail = second_ref[1024:1040].astype(F32)
        bb_ref[...] = tail[0:1] * scale_b
        ba_ref[...] = tail[1:2, :64] * scale_a

    @pl.when(core == 0)
    def _():
        put(mine_ref, other_ref)

    @pl.when(core == 1)
    def _():
        put(other_ref, mine_ref)


def spread_sum(shares_ref, out_ref):
    total = jnp.sum(shares_ref[...].astype(F32), axis=0, keepdims=True).astype(BF16)
    out_ref[...] = jnp.broadcast_to(total, out_ref.shape)


def input_grad(ga_ref, wa_ref, out_ref, f_ref, gx_ref, w_ref, at_ref):
    doubled(wa_ref, w_ref)
    banded_back_a(w_ref, at_ref)

    def stage(y, carry):
        for h in range(2):
            lanes = slice(h * 128, h * 128 + 128)
            f_ref[...] = ga_ref[:, y, :, lanes].astype(F32)
            for dx in range(3):
                gx_ref[dx, y, :, :, lanes] = f_ref[:, pl.ds(dx, 32), :].astype(BF16)
        return carry

    lax.fori_loop(0, 10, stage, 0)
    for h in range(2):
        parts = []
        for dx, dy in TAPS:
            for j in range(3):
                parts.append(gx_ref[dx, dy : dy + 8, 2 * h + j])
        lhs = jnp.concatenate(parts, axis=-1).reshape(256, 6912)
        value = lax.dot_general(lhs, at_ref[...], NT, preferred_element_type=F32)
        out_ref[:, h] = value.astype(BF16).reshape(8, 32, 256)


def swaps(axis):
    count = lax.axis_size(axis)
    near = [(i, i ^ 1) for i in range(count)]
    far = [(i, i + 1 if i % 2 else i - 1) for i in range(1, count - 1)]
    return near, far


def places():
    index = lax.axis_index(GZ)
    bits = tuple((1 - (index >> b) % 2).astype(jnp.uint32) for b in range(4))
    odd = tuple(lax.axis_index(axis) % 2 == 0 for axis in ("gx", "gy", GZ))
    return lax.axis_index(ALL).astype(jnp.int32).reshape(1), odd, bits


def halo(block, face, width, x_rows, evens):
    first, even, even_z = evens
    got = lax.ppermute(face, "gx", [(0, 1), (1, 0)])
    none = jnp.zeros_like(got)
    rest = jnp.zeros(block.shape[:2] + (x_rows - block.shape[2] - 2 * width,) + block.shape[3:], block.dtype)
    wide = jnp.concatenate([jnp.where(first, none, got), block, jnp.where(first, got, none), rest], axis=2)
    near, far = swaps("gy")
    low, high = wide[:width], wide[wide.shape[0] - width :]
    yfar = lax.ppermute(jnp.where(even, low, high), "gy", far)
    ynear = lax.ppermute(jnp.where(even, high, low), "gy", near)
    ylo, yhi = jnp.where(even, yfar, ynear), jnp.where(even, ynear, yfar)
    near, far = swaps(GZ)
    last = jnp.concatenate([ylo[:, 3:], wide[:, 3:], yhi[:, 3:]], axis=0)
    head = jnp.concatenate([ylo[:, :1], wide[:, :1], yhi[:, :1]], axis=0)
    zfar = lax.ppermute(jnp.where(even_z, head, last), GZ, far)
    znear = lax.ppermute(jnp.where(even_z, last, head), GZ, near)
    return wide, ynear, yfar, znear, zfar


CHIPS = ("gx", "gy", "gz_0")


def to_slabs(pieces, others):
    shape = pieces.shape
    zero = jnp.zeros((), jnp.uint32)
    for b, other in enumerate(others):
        pieces = pieces.reshape((16 >> (b + 1), 2, 1 << b) + shape[1:])
        start = (zero, other) + (zero,) * (pieces.ndim - 2)
        part = lax.dynamic_slice(pieces, start, pieces.shape[:1] + (1,) + pieces.shape[2:])
        got = lax.ppermute(part, GZ, [(i, i ^ (1 << b)) for i in range(16)])
        pieces = lax.dynamic_update_slice(pieces, got, start)
    return pieces.reshape(shape)


def on_device(volume, weight_a, bias_a, weight_b, bias_b, cotangent):
    cells_fine = 64 * 64 * 256
    scale_a = 1.0 / math.sqrt(cells_fine)
    scale_b = 1.0 / math.sqrt(cells_fine // 8)
    volume, cotangent, (where, evens, others) = lax.optimization_barrier((volume, cotangent, places()))

    v = call(
        in_rows, sds(8, 4, 32, 128), [pltpu.VMEM((2, 512, 32), F32)], jnp.transpose(volume, (0, 2, 3, 1)), flops=10**6
    )
    face = jnp.where(evens[0], v[:, :, 29:32], v[:, :, 0:3])
    sides = halo(v, face, 3, 40, evens)

    cot = jnp.transpose(cotangent[:, 0], (2, 1, 0)).reshape(16, 8, 4, 128)
    cot = lax.all_to_all(cot, GZ, 0, 0, tiled=True)
    cot = jnp.transpose(cot.reshape(16, 4, 2, 4, 128), (3, 1, 0, 2, 4)).reshape(4, 4, 16, 256)

    wa27 = weight_a.reshape(27, 32, 64)
    wb27 = weight_b.reshape(27, 64, 128)

    m_a = call(banded_ahead_a, sds(2304, 256), [pltpu.VMEM((27, 32, 128), BF16)], wa27, flops=10**7)

    feat, grad_b, sum_b, px, face_b, vo, slope = call(
        forward,
        (
            sds(4, 4, 16, 256), sds(4, 4, 16, 256), sds(1, 128, dtype=F32), sds(3, 6, 5, 16, 128), sds(4, 4, 2, 256),
            pltpu.HBM((10, 6, 40, 128), BF16), pltpu.HBM((5, 10, 48, 256), BF16),
        ),
        [
            pltpu.VMEM((4, 56, 128), F32), pltpu.VMEM((3, 14, 6, 48, 128), BF16),
            pltpu.VMEM((6, 48, 128), F32), pltpu.VMEM((6, 24, 128), F32), pltpu.VMEM((4, 4, 16, 128), F32),
            pltpu.VMEM((2304, 256), BF16),
            pltpu.VMEM((10, 6, 40, 128), BF16), pltpu.VMEM((5, 10, 48, 256), BF16), pltpu.SemaphoreType.DMA((6,)),
        ],
        where, *sides, m_a, bias_a.reshape(1, 64), wb27, bias_b.reshape(1, 128), cot,
        flops=2 * 10**9, room=24, far_outs=2,
    )

    sides_b = halo(grad_b, face_b, 2, 24, evens)
    wb = call(weight_b_terms, sds(27, 64, 128), [], px, grad_b, flops=10**9)

    out = jnp.transpose(feat.reshape(4, 4, 16, 2, 128), (2, 1, 3, 0, 4)).reshape(16, 8, 4, 128)

    keep, send, ga = call(
        backward,
        (sds(1280, 128), sds(1280, 128), pltpu.HBM((5, 10, 40, 256), BF16)),
        [
            pltpu.VMEM((2, 4, 40, 128), F32), pltpu.VMEM((3, 8, 6, 32, 256), BF16),
            pltpu.VMEM((6, 48, 128), F32), pltpu.VMEM((10, 48, 128), F32), pltpu.VMEM((8, 5, 32, 256), BF16),
            pltpu.VMEM((2560, 128), BF16), pltpu.VMEM((3, 10, 6, 32, 128), BF16), pltpu.VMEM((6, 40, 128), F32),
            pltpu.VMEM((256, 4608), BF16),
            pltpu.VMEM((5, 10, 40, 256), BF16), pltpu.SemaphoreType.DMA((5,)),
        ],
        where, *sides_b, wb27, wb, sum_b, slope, vo, flops=2 * 10**9, room=24, far_outs=1,
    )

    flip = [(0, 1), (1, 0)]
    count = lax.axis_size(CHIPS)
    got = lax.ppermute(send, "gz_1", flip)
    chip = (keep.astype(F32) + got.astype(F32)).astype(BF16)
    shares = lax.all_to_all(chip.reshape(count, 5, 2, 128), CHIPS, 0, 0, tiled=True)
    spread = call(spread_sum, sds(count, 5, 2, 128), [], shares, flops=10**6)
    mine = lax.all_to_all(spread, CHIPS, 0, 0, tiled=True).reshape(count * 10, 128)
    other = lax.ppermute(mine, "gz_1", flip)
    features = jnp.transpose(to_slabs(out, others).reshape(128, 4, 128), (2, 1, 0)).reshape(128, 1, 4, 128)

    gi = call(
        input_grad, sds(8, 2, 32, 256), [pltpu.VMEM((5, 40, 128), F32), pltpu.VMEM((3, 10, 5, 32, 256), BF16),
         pltpu.VMEM((27, 32, 128), BF16), pltpu.VMEM((256, 6912), BF16)],
        ga, wa27, flops=2 * 10**9, room=16,
    )
    gi = jnp.transpose(gi.reshape(8, 2, 32, 8, 32), (4, 2, 0, 1, 3)).reshape(32, 32, 8, 16)

    total_wa, total_ba, total_wb, total_bb = call(
        functools.partial(finish, scale_a, scale_b),
        (sds(27, 32, 64, dtype=F32), sds(1, 64, dtype=F32), sds(1728, 128, dtype=F32), sds(1, 128, dtype=F32)),
        [], where, mine, other, flops=10**6,
    )
    return (
        features,
        gi,
        total_wa.reshape(3, 3, 3, 32, 64),
        total_ba.reshape(64),
        total_wb.reshape(3, 3, 3, 64, 128),
        total_bb.reshape(128),
    )


def solution(mesh):
    finer = Mesh(
        mesh.devices.reshape(mesh.shape["gx"], mesh.shape["gy"], 8, 2), ("gx", "gy", "gz_0", "gz_1")
    )
    return jax.shard_map(
        on_device,
        mesh=finer,
        in_specs=(P(None, "gx", "gy", GZ), P(), P(), P(), P(), P(None, GX_GZ, "gy", None)),
        out_specs=(P(None, GX_GZ, "gy", None), P(None, "gx", "gy", GZ), P(), P(), P(), P()),
        check_vma=False,
    )
```

```python
import functools
import math

import jax
import jax.numpy as jnp
from jax import lax
from jax.experimental import pallas as pl
from jax.experimental.pallas import tpu as pltpu
from jax.sharding import Mesh
from jax.sharding import PartitionSpec as P

ALL = ("gx", "gy", "gz_0", "gz_1")
GZ = ("gz_0", "gz_1")
GX_GZ = ("gx", "gz_0", "gz_1")
BF16 = jnp.bfloat16
F32 = jnp.float32
TAPS = [(dx, dy) for dx in range(3) for dy in range(3)]


def call(body, outs, scratch, *args, flops=10**8, room=8, far_args=0, far_outs=0):
    vmem = pl.BlockSpec(memory_space=pltpu.VMEM)
    smem = pl.BlockSpec(memory_space=pltpu.SMEM)
    far = pl.BlockSpec(memory_space=pltpu.HBM)
    near = [smem if a.dtype == jnp.int32 else vmem for a in args[: len(args) - far_args]]
    if isinstance(outs, tuple):
        out_specs = (vmem,) * (len(outs) - far_outs) + (far,) * far_outs
    else:
        out_specs = vmem
    return pl.pallas_call(
        body,
        out_shape=outs,
        in_specs=near + [far] * far_args,
        out_specs=out_specs,
        scratch_shapes=scratch,
        compiler_params=pltpu.CompilerParams(vmem_limit_bytes=room * 2**20),
        cost_estimate=pl.CostEstimate(flops=flops, bytes_accessed=10**6, transcendentals=0),
    )(*args)


def sds(*shape, dtype=BF16):
    return jax.ShapeDtypeStruct(shape, dtype)


def doubled(w_ref, out_ref):
    w = w_ref[...].astype(F32)
    out_ref[...] = jnp.concatenate([w, w], axis=-1).astype(BF16)


def blocks(wa_ref, wb_ref):
    low = lax.broadcasted_iota(jnp.int32, (32, 128), 1) < 64
    zero_a = jnp.zeros((32, 128), BF16)
    zero_b = jnp.zeros((64, 128), BF16)

    def wa(dx, dy, dz):
        return wa_ref[(dx * 3 + dy) * 3 + dz] if 0 <= dz <= 2 else zero_a

    def wb(dx, dy, dz):
        return wb_ref[(dx * 3 + dy) * 3 + dz] if 0 <= dz <= 2 else zero_b

    def pair(first, second):
        return jnp.where(low, first.astype(F32), second.astype(F32)).astype(BF16)

    return wa, wb, pair, zero_b


def banded_ahead_a(w_ref, a_ref, double_ref):
    doubled(w_ref, double_ref)
    wa, _, pair, _ = blocks(double_ref, None)
    for t, (dx, dy) in enumerate(TAPS):
        for zi in range(8):
            for p in range(2):
                a_ref[t * 256 + zi * 32 : t * 256 + zi * 32 + 32, p * 128 : p * 128 + 128] = pair(
                    wa(dx, dy, zi - 2 * p - 1), wa(dx, dy, zi - 2 * p - 2)
                )


def banded_ahead_b(wb_ref, b_ref):
    _, wb, _, _ = blocks(None, wb_ref)
    for t, (dx, dy) in enumerate(TAPS):
        for zi in range(4):
            for zo in range(2):
                b_ref[t * 256 + zi * 64 : t * 256 + zi * 64 + 64, zo * 128 : zo * 128 + 128] = wb(dx, dy, zi - zo)


def banded_back_b(wb_ref, bt_ref):
    _, wb, _, zero_b = blocks(None, wb_ref)
    for t, (dx, dy) in enumerate(TAPS):
        for z in range(4):
            for zi in range(4):
                dz = zi - z // 2
                block = wb(2 - dx, 2 - dy, 2 - dz) if 0 <= dz <= 2 else zero_b
                bt_ref[z * 64 : z * 64 + 64, t * 512 + zi * 128 : t * 512 + zi * 128 + 128] = block


def banded_back_a(wa_ref, at_ref):
    wa, _, pair, _ = blocks(wa_ref, None)
    for t, (dx, dy) in enumerate(TAPS):
        for z in range(8):
            for p in range(6):
                dz = 2 * p - z - 1
                at_ref[z * 32 : z * 32 + 32, t * 768 + p * 128 : t * 768 + p * 128 + 128] = pair(
                    wa(2 - dx, 2 - dy, 2 - dz), wa(2 - dx, 2 - dy, 1 - dz)
                )


def position(where_ref):
    code = where_ref[0]
    return code // 128, (code // 16) % 8, code % 16


def iota(shape, dim):
    return lax.broadcasted_iota(jnp.int32, shape, dim)


def sigmoid_of(value):
    return 0.5 * jnp.tanh(0.5 * value) + 0.5


def in_rows(v_ref, out_ref, f_ref):
    for y in range(8):
        f_ref[y % 2] = v_ref[:, y].astype(F32).reshape(512, 32)
        for q in range(4):
            columns = [f_ref[y % 2, pl.ds(4 * q + z, 32, stride=16), :] for z in range(4)]
            out_ref[y, q] = jnp.concatenate(columns, axis=0).T.astype(BF16)


def forward(
    where_ref, v_ref, ynear_ref, yfar_ref, znear_ref, zfar_ref, a_ref, bias_a_ref, wb_ref, bias_b_ref, cot_ref,
    feat_ref, grad_ref, sum_ref, px_ref, face_ref, vo_hbm, slope_hbm,
    f_ref, vx_ref, s_ref, p_ref, g_ref, b_ref, vo_ref, slope_ref, sem,
):
    banded_ahead_b(wb_ref, b_ref)
    twice = jnp.concatenate([bias_a_ref[...], bias_a_ref[...]], axis=-1)
    bias_a = jnp.concatenate([twice, twice], axis=-1)
    bias_b = jnp.concatenate([bias_b_ref[...], bias_b_ref[...]], axis=-1)
    gx, gy, gz = position(where_ref)

    def stage(src, rows, y0, q0, nq):
        def step(y, carry):
            f_ref[0:nq, 0:40, :] = src[y].astype(F32)
            for dx in range(3):
                vx_ref[dx, y0 + y, pl.ds(q0, nq)] = f_ref[0:nq, pl.ds(dx, 48), :].astype(BF16)

            @pl.when(jnp.logical_and(y0 + y >= 2, y0 + y < 12))
            def _():
                vo_ref[y0 + y - 2, pl.ds(q0, nq)] = f_ref[0:nq, pl.ds(2, 40), :].astype(BF16)

            return carry

        lax.fori_loop(0, rows, step, 0)

    even_y, even_z = gy % 2 == 0, gz % 2 == 0
    stage(v_ref, 8, 3, 1, 4)
    stage(ynear_ref, 3, jnp.where(even_y, 11, 0), 1, 4)
    stage(yfar_ref, 3, jnp.where(even_y, 0, 11), 1, 4)
    stage(znear_ref, 14, 0, jnp.where(even_z, 5, 0), 1)
    stage(zfar_ref, 14, 0, jnp.where(even_z, 0, 5), 1)

    save_vo = pltpu.make_async_copy(vo_ref, vo_hbm, sem.at[5])
    save_vo.start()

    def save_slope(q):
        return pltpu.make_async_copy(slope_ref.at[q], slope_hbm.at[q], sem.at[q])

    fold = iota((6, 48, 128), 2) < 64
    shape = (6, 24, 128)
    x = iota(shape, 1) + (gx * 16 - 1)
    y = iota(shape, 0) + (gy * 4 - 1)
    zlane = iota(shape, 2) // 64
    inside_xy = (x >= 0) & (x < 32) & (y >= 0) & (y < 32)

    def conv_a(q, carry):
        parts = []
        for dx, dy in TAPS:
            parts.append(vx_ref[dx, dy : dy + 12, q])
            parts.append(vx_ref[dx, dy : dy + 12, q + 1])
        lhs = jnp.concatenate(parts, axis=-1).reshape(576, 2304)
        before = jnp.dot(lhs, a_ref[...], preferred_element_type=F32) + bias_a
        s = sigmoid_of(before)
        slope = (0.125 * (s * (1.0 + before * (1.0 - s)))).astype(BF16)
        slope_ref[q] = slope.reshape(12, 48, 256)[1:11]
        save_slope(q).start()
        act = (before * s).reshape(6, 2, 48, 256)
        rows = act[:, 0] + act[:, 1]
        lo, hi = rows[..., :128], rows[..., 128:]
        lo = lo + pltpu.roll(lo, 64, 2)
        hi = hi + pltpu.roll(hi, 64, 2)
        s_ref[q % 2] = jnp.where(fold, lo, hi)
        mean = (s_ref[q % 2, :, pl.ds(0, 24, stride=2), :] + s_ref[q % 2, :, pl.ds(1, 24, stride=2), :]) * 0.125
        z = zlane + (gz * 8 - 1 + 2 * q)
        p_ref[q % 2] = jnp.where(inside_xy & (z >= 0) & (z < 128), mean, 0.0)
        for dx in range(3):
            px_ref[dx, :, q] = p_ref[q % 2, :, pl.ds(dx, 16), :].astype(BF16)
        return carry

    for q in range(5):
        conv_a(q, 0)

    parts = []
    for dx, dy in TAPS:
        parts.append(px_ref[dx, dy : dy + 4, 0:4])
        parts.append(px_ref[dx, dy : dy + 4, 1:5])
    lhs = jnp.concatenate(parts, axis=-1).reshape(256, 2304)
    before = jnp.dot(lhs, b_ref[...], preferred_element_type=F32) + bias_b
    s = sigmoid_of(before)
    feat_ref[...] = (before * s).astype(BF16).reshape(4, 4, 16, 256)
    cot = cot_ref[...].reshape(256, 256).astype(F32)
    grad = (cot * (s * (1.0 + before * (1.0 - s)))).astype(BF16)
    grad_ref[...] = grad.reshape(4, 4, 16, 256)
    wide = grad.astype(F32)
    total = jnp.sum(wide, axis=0, keepdims=True)
    sum_ref[...] = total[:, :128] + total[:, 128:]
    for h in range(2):
        lanes = slice(h * 128, h * 128 + 128)
        g_ref[...] = wide[:, lanes].reshape(4, 4, 16, 128)
        face_ref[..., lanes] = jnp.where(gx == 0, g_ref[:, :, pl.ds(14, 2), :], g_ref[:, :, pl.ds(0, 2), :]).astype(BF16)
    for q in range(5):
        save_slope(q).wait()
    save_vo.wait()


TN = (((0,), (0,)), ((), ()))
NT = (((1,), (1,)), ((), ()))


def weight_b_terms(px_ref, grad_ref, out_ref):
    grad = grad_ref[...].reshape(256, 256)
    for t, (dx, dy) in enumerate(TAPS):
        cells = jnp.concatenate([px_ref[dx, dy : dy + 4, 0:4], px_ref[dx, dy : dy + 4, 1:5]], axis=-1)
        terms = lax.dot_general(cells.reshape(256, 256), grad, TN, preferred_element_type=F32)
        for dz in range(3):
            out_ref[3 * t + dz] = (
                terms[dz * 64 : dz * 64 + 64, :128] + terms[dz * 64 + 64 : dz * 64 + 128, 128:]
            ).astype(BF16)


def backward(
    where_ref, g_ref, ynear_ref, yfar_ref, znear_ref, zfar_ref, w_ref, wb_ref, sum_b_ref, slope_ref, vo_ref,
    keep_ref, send_ref, ga_hbm,
    rows_ref, s_ref, t_ref, own_ref, flat_ref, vx_ref, v_ref, bt_ref, ga_ref, sem,
):
    banded_back_b(w_ref, bt_ref)
    gx, gy, gz = position(where_ref)

    even_y, even_z = gy % 2 == 0, gz % 2 == 0

    def put(src, base):
        for y in range(src.shape[0]):
            start = pl.multiple_of(base + 24 * y, 8)
            rows_ref[1:5, pl.ds(start, 24), :] = src[y].astype(F32)

    put(g_ref, 48)
    put(ynear_ref, jnp.where(even_y, 144, 0))
    put(yfar_ref, jnp.where(even_y, 0, 144))
    for src, q in ((znear_ref, jnp.where(even_z, 5, 0)), (zfar_ref, jnp.where(even_z, 0, 5))):
        for y in range(8):
            rows_ref[pl.ds(q, 1), 24 * y : 24 * y + 24, :] = src[y].astype(F32)

    def stage_v(y, carry):
        groups = vo_ref[y].astype(F32)
        v_ref[...] = jnp.where(
            iota((5, 40, 128), 2) < 64, pltpu.roll(groups[0:5], 64, 2), pltpu.roll(groups[1:6], 64, 2)
        )
        for dx in range(3):
            vx_ref[dx, y] = v_ref[:, pl.ds(dx, 32), :].astype(BF16)
        return carry

    lax.fori_loop(0, 10, stage_v, 0)

    shape = (10, 48, 128)
    x = iota(shape, 1) + (gx * 32 - 2)
    y = iota(shape, 0) + (gy * 8 - 1)
    zlane = iota(shape, 2) // 64
    inside_xy = (x >= 0) & (x < 64) & (y >= 0) & (y < 64)

    parts = []
    for dx, dy in TAPS:
        for j in range(2):
            parts.append(rows_ref[j : j + 5, pl.ds(24 * dy + dx, 144), :].astype(BF16))
    lhs = jnp.concatenate(parts, axis=-1).reshape(720, 4608)
    back = lax.dot_general(lhs, bt_ref[...], NT, preferred_element_type=F32)

    def save_ga(q):
        return pltpu.make_async_copy(ga_ref.at[q], ga_hbm.at[q], sem.at[q])

    def conv_b(q, total):
        pooled = back[144 * q : 144 * q + 144].astype(BF16).astype(F32).reshape(6, 24, 256)
        sums = []
        for h in range(2):
            half = pooled[..., h * 128 : h * 128 + 128]
            slot = 2 * (q % 2) + h
            s_ref[slot, :, pl.ds(0, 24, stride=2), :] = half
            s_ref[slot, :, pl.ds(1, 24, stride=2), :] = half
            spread = jnp.broadcast_to(s_ref[slot].reshape(6, 1, 48, 128), (6, 2, 48, 128)).reshape(12, 48, 128)[1:11]
            z = zlane + (gz * 16 - 2 + 4 * q + 2 * h)
            slope = slope_ref[q, :, :, h * 128 : h * 128 + 128].astype(F32)
            t_ref[slot] = jnp.where(inside_xy & (z >= 0) & (z < 256), spread * slope, 0.0)
            ga_ref[q, :, :, h * 128 : h * 128 + 128] = t_ref[slot, :, pl.ds(1, 40), :].astype(BF16)
            own = t_ref[slot, 1:9, pl.ds(2, 32), :].astype(BF16)
            own_ref[:, q + h, :, 128 - h * 128 : 256 - h * 128] = own
            keep = 0.0 if q == 4 * h else 1.0
            sums.append(keep * jnp.sum(own.astype(F32).reshape(256, 128), axis=0, keepdims=True))
        save_ga(q).start()
        return total + sums[0] + sums[1]

    total = jnp.zeros((1, 128), F32)
    for q in range(5):
        total = conv_b(q, total)
    flat_ref[0:1728] = wb_ref[...].reshape(1728, 128)
    row = iota((16, 128), 0)
    sums = jnp.where(row == 0, sum_b_ref[...], jnp.where(row == 1, total + pltpu.roll(total, 64, 1), 0.0))
    flat_ref[2304:2320] = sums.astype(BF16)
    flat_ref[2320:2560] = jnp.zeros((240, 128), BF16)

    flat = own_ref[:, 1:5].reshape(1024, 256).T
    for t, (dx, dy) in enumerate(TAPS):
        cells = jnp.concatenate([vx_ref[dx, dy : dy + 8, 0:4], vx_ref[dx, dy : dy + 8, 1:5]], axis=-1)
        terms = jnp.dot(flat, cells.reshape(1024, 256), preferred_element_type=F32)
        block = terms[0:64]
        for zo in range(1, 4):
            block = block + pltpu.roll(terms[zo * 64 : zo * 64 + 64], 256 - 32 * zo, 1)
        flat_ref[1728 + 64 * t : 1792 + 64 * t] = block[:, :128].astype(BF16)

    half = pl.multiple_of((gz % 2) * 1280, 1280)
    rest = pl.multiple_of((1 - gz % 2) * 1280, 1280)
    keep_ref[...] = flat_ref[pl.ds(half, 1280), :]
    send_ref[...] = flat_ref[pl.ds(rest, 1280), :]
    for q in range(5):
        save_ga(q).wait()


def finish(scale_a, scale_b, where_ref, mine_ref, other_ref, wa_ref, ba_ref, wb_ref, bb_ref):
    core = where_ref[0] % 2

    def put(first_ref, second_ref):
        wb_ref[0:1280] = first_ref[...].astype(F32) * scale_b
        wb_ref[1280:1728] = second_ref[0:448].astype(F32) * scale_b
        for t in range(9):
            block = second_ref[448 + 64 * t : 512 + 64 * t].astype(F32).T * scale_a
            for dz in range(3):
                wa_ref[3 * t + dz] = block[32 + 32 * dz : 64 + 32 * dz]
        tail = second_ref[1024:1040].astype(F32)
        bb_ref[...] = tail[0:1] * scale_b
        ba_ref[...] = tail[1:2, :64] * scale_a

    @pl.when(core == 0)
    def _():
        put(mine_ref, other_ref)

    @pl.when(core == 1)
    def _():
        put(other_ref, mine_ref)


def spread_sum(shares_ref, out_ref):
    total = jnp.sum(shares_ref[...].astype(F32), axis=0, keepdims=True).astype(BF16)
    out_ref[...] = jnp.broadcast_to(total, out_ref.shape)


def input_grad(ga_ref, wa_ref, out_ref, f_ref, gx_ref, w_ref, at_ref):
    doubled(wa_ref, w_ref)
    banded_back_a(w_ref, at_ref)

    def stage(y, carry):
        for h in range(2):
            lanes = slice(h * 128, h * 128 + 128)
            f_ref[...] = ga_ref[:, y, :, lanes].astype(F32)
            for dx in range(3):
                gx_ref[dx, y, :, :, lanes] = f_ref[:, pl.ds(dx, 32), :].astype(BF16)
        return carry

    lax.fori_loop(0, 10, stage, 0)
    for h in range(2):
        parts = []
        for dx, dy in TAPS:
            for j in range(3):
                parts.append(gx_ref[dx, dy : dy + 8, 2 * h + j])
        lhs = jnp.concatenate(parts, axis=-1).reshape(256, 6912)
        value = lax.dot_general(lhs, at_ref[...], NT, preferred_element_type=F32)
        out_ref[:, h] = value.astype(BF16).reshape(8, 32, 256)


def swaps(axis):
    count = lax.axis_size(axis)
    near = [(i, i ^ 1) for i in range(count)]
    far = [(i, i + 1 if i % 2 else i - 1) for i in range(1, count - 1)]
    return near, far


def places():
    index = lax.axis_index(GZ)
    bits = tuple((1 - (index >> b) % 2).astype(jnp.uint32) for b in range(4))
    odd = tuple(lax.axis_index(axis) % 2 == 0 for axis in ("gx", "gy", GZ))
    return lax.axis_index(ALL).astype(jnp.int32).reshape(1), odd, bits


def halo(block, face, width, x_rows, evens):
    first, even, even_z = evens
    got = lax.ppermute(face, "gx", [(0, 1), (1, 0)])
    none = jnp.zeros_like(got)
    rest = jnp.zeros(block.shape[:2] + (x_rows - block.shape[2] - 2 * width,) + block.shape[3:], block.dtype)
    wide = jnp.concatenate([jnp.where(first, none, got), block, jnp.where(first, got, none), rest], axis=2)
    near, far = swaps("gy")
    low, high = wide[:width], wide[wide.shape[0] - width :]
    yfar = lax.ppermute(jnp.where(even, low, high), "gy", far)
    ynear = lax.ppermute(jnp.where(even, high, low), "gy", near)
    ylo, yhi = jnp.where(even, yfar, ynear), jnp.where(even, ynear, yfar)
    near, far = swaps(GZ)
    last = jnp.concatenate([ylo[:, 3:], wide[:, 3:], yhi[:, 3:]], axis=0)
    head = jnp.concatenate([ylo[:, :1], wide[:, :1], yhi[:, :1]], axis=0)
    zfar = lax.ppermute(jnp.where(even_z, head, last), GZ, far)
    znear = lax.ppermute(jnp.where(even_z, last, head), GZ, near)
    return wide, ynear, yfar, znear, zfar


CHIPS = ("gx", "gy", "gz_0")


def to_slabs(pieces, others):
    shape = pieces.shape
    zero = jnp.zeros((), jnp.uint32)
    for b, other in enumerate(others):
        pieces = pieces.reshape((16 >> (b + 1), 2, 1 << b) + shape[1:])
        start = (zero, other) + (zero,) * (pieces.ndim - 2)
        part = lax.dynamic_slice(pieces, start, pieces.shape[:1] + (1,) + pieces.shape[2:])
        got = lax.ppermute(part, GZ, [(i, i ^ (1 << b)) for i in range(16)])
        pieces = lax.dynamic_update_slice(pieces, got, start)
    return pieces.reshape(shape)


def on_device(volume, weight_a, bias_a, weight_b, bias_b, cotangent):
    cells_fine = 64 * 64 * 256
    scale_a = 1.0 / math.sqrt(cells_fine)
    scale_b = 1.0 / math.sqrt(cells_fine // 8)
    volume, cotangent, (where, evens, others) = lax.optimization_barrier((volume, cotangent, places()))

    v = call(
        in_rows, sds(8, 4, 32, 128), [pltpu.VMEM((2, 512, 32), F32)], jnp.transpose(volume, (0, 2, 3, 1)), flops=10**6
    )
    face = jnp.where(evens[0], v[:, :, 29:32], v[:, :, 0:3])
    sides = halo(v, face, 3, 40, evens)

    cot = jnp.transpose(cotangent[:, 0], (2, 1, 0)).reshape(16, 8, 4, 128)
    cot = lax.all_to_all(cot, GZ, 0, 0, tiled=True)
    cot = jnp.transpose(cot.reshape(16, 4, 2, 4, 128), (3, 1, 0, 2, 4)).reshape(4, 4, 16, 256)

    wa27 = weight_a.reshape(27, 32, 64)
    wb27 = weight_b.reshape(27, 64, 128)

    m_a = call(banded_ahead_a, sds(2304, 256), [pltpu.VMEM((27, 32, 128), BF16)], wa27, flops=10**7)

    feat, grad_b, sum_b, px, face_b, vo, slope = call(
        forward,
        (
            sds(4, 4, 16, 256), sds(4, 4, 16, 256), sds(1, 128, dtype=F32), sds(3, 6, 5, 16, 128), sds(4, 4, 2, 256),
            pltpu.HBM((10, 6, 40, 128), BF16), pltpu.HBM((5, 10, 48, 256), BF16),
        ),
        [
            pltpu.VMEM((4, 56, 128), F32), pltpu.VMEM((3, 14, 6, 48, 128), BF16),
            pltpu.VMEM((2, 6, 48, 128), F32), pltpu.VMEM((2, 6, 24, 128), F32), pltpu.VMEM((4, 4, 16, 128), F32),
            pltpu.VMEM((2304, 256), BF16),
            pltpu.VMEM((10, 6, 40, 128), BF16), pltpu.VMEM((5, 10, 48, 256), BF16), pltpu.SemaphoreType.DMA((6,)),
        ],
        where, *sides, m_a, bias_a.reshape(1, 64), wb27, bias_b.reshape(1, 128), cot,
        flops=2 * 10**9, room=24, far_outs=2,
    )

    sides_b = halo(grad_b, face_b, 2, 24, evens)
    wb = call(weight_b_terms, sds(27, 64, 128), [], px, grad_b, flops=10**9)

    out = jnp.transpose(feat.reshape(4, 4, 16, 2, 128), (2, 1, 3, 0, 4)).reshape(16, 8, 4, 128)

    keep, send, ga = call(
        backward,
        (sds(1280, 128), sds(1280, 128), pltpu.HBM((5, 10, 40, 256), BF16)),
        [
            pltpu.VMEM((6, 200, 256), F32),
            pltpu.VMEM((4, 6, 48, 128), F32), pltpu.VMEM((4, 10, 48, 128), F32), pltpu.VMEM((8, 6, 32, 256), BF16),
            pltpu.VMEM((2560, 128), BF16), pltpu.VMEM((3, 10, 5, 32, 128), BF16), pltpu.VMEM((5, 40, 128), F32),
            pltpu.VMEM((256, 4608), BF16),
            pltpu.VMEM((5, 10, 40, 256), BF16), pltpu.SemaphoreType.DMA((5,)),
        ],
        where, *sides_b, wb27, wb, sum_b, slope, vo, flops=2 * 10**9, room=32, far_outs=1,
    )

    flip = [(0, 1), (1, 0)]
    count = lax.axis_size(CHIPS)
    got = lax.ppermute(send, "gz_1", flip)
    chip = (keep.astype(F32) + got.astype(F32)).astype(BF16)
    shares = lax.all_to_all(chip.reshape(count, 5, 2, 128), CHIPS, 0, 0, tiled=True)
    spread = call(spread_sum, sds(count, 5, 2, 128), [], shares, flops=10**6)
    mine = lax.all_to_all(spread, CHIPS, 0, 0, tiled=True).reshape(count * 10, 128)
    other = lax.ppermute(mine, "gz_1", flip)
    features = jnp.transpose(to_slabs(out, others).reshape(128, 4, 128), (2, 1, 0)).reshape(128, 1, 4, 128)

    gi = call(
        input_grad, sds(8, 2, 32, 256), [pltpu.VMEM((5, 40, 128), F32), pltpu.VMEM((3, 10, 5, 32, 256), BF16),
         pltpu.VMEM((27, 32, 128), BF16), pltpu.VMEM((256, 6912), BF16)],
        ga, wa27, flops=2 * 10**9, room=16,
    )
    gi = jnp.transpose(gi.reshape(8, 2, 32, 8, 32), (4, 2, 0, 1, 3)).reshape(32, 32, 8, 16)

    total_wa, total_ba, total_wb, total_bb = call(
        functools.partial(finish, scale_a, scale_b),
        (sds(27, 32, 64, dtype=F32), sds(1, 64, dtype=F32), sds(1728, 128, dtype=F32), sds(1, 128, dtype=F32)),
        [], where, mine, other, flops=10**6,
    )
    return (
        features,
        gi,
        total_wa.reshape(3, 3, 3, 32, 64),
        total_ba.reshape(64),
        total_wb.reshape(3, 3, 3, 64, 128),
        total_bb.reshape(128),
    )


def solution(mesh):
    finer = Mesh(
        mesh.devices.reshape(mesh.shape["gx"], mesh.shape["gy"], 8, 2), ("gx", "gy", "gz_0", "gz_1")
    )
    return jax.shard_map(
        on_device,
        mesh=finer,
        in_specs=(P(None, "gx", "gy", GZ), P(), P(), P(), P(), P(None, GX_GZ, "gy", None)),
        out_specs=(P(None, GX_GZ, "gy", None), P(None, "gx", "gy", GZ), P(), P(), P(), P()),
        check_vma=False,
    )
```
